256 devices in a mesh: dp: 64 (over y, z_hi, x), tensor: 4 (over z_lo, core).
Axes of the slice: x: 4, y: 4, z: 8 (z_hi: 4, z_lo: 2; z = z_hi * 2 + z_lo), core: 2. Of those that a mesh axis runs over, the one named last changes fastest.
Arguments:
- activations: bfloat16 [32768, 4096], P('dp'), may hold values from -1000 to 1000
- norm_gain: bfloat16 [4096], replicated, may hold values from 0.5 to 1.5
- query_blocks: bfloat16 [128, 32, 4096], P('dp', None, 'tensor'), may hold values from -64 to 64
- query_scales: int32 [128, 1, 4096], P('dp', None, 'tensor'), may hold values from -9 to -5
- key_blocks: bfloat16 [128, 32, 512], P('dp', None, 'tensor'), may hold values from -64 to 64
- key_scales: int32 [128, 1, 512], P('dp', None, 'tensor'), may hold values from -9 to -5
- value_blocks: bfloat16 [128, 32, 512], P('dp', None, 'tensor'), may hold values from -6 to 6
- value_scales: int32 [128, 1, 512], P('dp', None, 'tensor'), may hold values from -9 to -5
- output_blocks: bfloat16 [128, 32, 4096], P('tensor', None, 'dp'), may hold values from -6 to 6
- output_scales: int32 [128, 1, 4096], P('tensor', None, 'dp'), may hold values from -9 to -5
Outputs:
- attended: bfloat16 [32768, 4096], P('dp')
The draws below stay inside these ranges and needn't reach their ends.
All inputs are finite; a program needn't handle non-finite values.
Results may differ from the reference program's by a relative error of at most 0.015.
The reference program's roundings to bfloat16 on the way count: a program that leaves them out, or rounds other values in their place, can miss the bound.
Values may be sent and summed in bfloat16 or wider, within the bound.
A program may use at most 128 MiB of HBM per device.

```python
import math
import jax
import jax.numpy as jnp
from jax import lax

D = 4096
HEADS = 32
KV_HEADS = 4
HEAD_DIM = 128
BLOCK = 32
SEQ = 256
SEQS = 2
TOKENS = 32768
N_DP = 64
N_TENSOR = 4


def exponent_field(key, shape):
    return jax.random.randint(key, shape, -9, -4).astype(jnp.int32)


def drawn_blocks(key, salt, columns):
    scales = exponent_field(jax.random.fold_in(key, salt), (D // BLOCK, 1, columns))
    values = jnp.clip(jax.random.normal(jax.random.fold_in(key, salt + 1), (D // BLOCK, BLOCK, columns), jnp.float32), -6.0, 6.0)
    return (scales, values)


def draw_query_scales(key, part):
    return drawn_blocks(key, 11, HEADS * HEAD_DIM)[0]


def draw_query_blocks(key, part):
    return drawn_blocks(key, 11, HEADS * HEAD_DIM)[1].astype(jnp.bfloat16)


def draw_key_scales(key, part):
    return drawn_blocks(key, 21, KV_HEADS * HEAD_DIM)[0]


def draw_key_blocks(key, part):
    return drawn_blocks(key, 21, KV_HEADS * HEAD_DIM)[1].astype(jnp.bfloat16)


def draw_activations(key, part):
    row_scale = jnp.exp(jax.random.uniform(jax.random.fold_in(key, 31), (TOKENS, 1), jnp.float32, 0.0, math.log(10.0)))
    column_scale = jnp.exp(jax.random.uniform(jax.random.fold_in(key, 32), (1, D), jnp.float32, 0.0, math.log(10.0)))
    base = jnp.clip(jax.random.normal(jax.random.fold_in(key, 33), (TOKENS, D), jnp.float32), -6.0, 6.0) * row_scale * column_scale
    return base.astype(jnp.bfloat16)


def set_ends(drawn, rng, low, top_value):
    longest = drawn.shape.index(max(drawn.shape))
    spots = []
    for shift in (0, 1):
        where = [jax.random.randint(jax.random.fold_in(rng, axis), (), 0, length) for axis, length in enumerate(drawn.shape)]
        where[longest] = (where[longest] + shift) % drawn.shape[longest]
        spots.append(tuple(where))
    return drawn.at[spots[0]].set(low).at[spots[1]].set(top_value)


def level_of(key, extent, shards, least, high):
    gain = 1.0
    for axis_at, parts in shards:
        heights = jax.random.uniform(jax.random.fold_in(jax.random.fold_in(key, 6), axis_at), (parts,), jnp.float32, least / len(shards), high / len(shards))
        gain = gain * jnp.repeat(jnp.exp(heights), extent[axis_at] // parts).reshape((-1,) + (1,) * (len(extent) - 1 - axis_at))
    return gain


def gaussian(key, shape, width, reach, cuts=(), kind=jnp.bfloat16):
    array = width * jax.random.normal(key, shape, jnp.float32)
    if cuts:
        array = array * level_of(key, shape, cuts, -0.22, 0.18)
    return jnp.clip(array, -reach, reach).astype(kind)


def setup_inputs(seed: int = 0) -> dict:
    splits = jax.random.split(jax.random.key(seed), 11)
    activations = draw_activations(jax.random.fold_in(splits[10], 71), 0)
    norm_gain = jnp.clip(1.0 + 0.1 * jax.random.normal(splits[1], (D,), jnp.float32), 0.5, 1.5).astype(jnp.bfloat16)
    query_blocks = draw_query_blocks(jax.random.fold_in(splits[10], 71), 0)
    query_scales = draw_query_scales(jax.random.fold_in(splits[10], 71), 0)
    key_blocks = draw_key_blocks(jax.random.fold_in(splits[10], 71), 0)
    key_scales = draw_key_scales(jax.random.fold_in(splits[10], 71), 0)
    value_blocks = gaussian(splits[6], (D // BLOCK, BLOCK, KV_HEADS * HEAD_DIM), 1.0, 6.0, ((0, 64), (2, 4)))
    value_scales = set_ends(jax.random.randint(splits[7], (D // BLOCK, 1, KV_HEADS * HEAD_DIM), -9, -4), jax.random.fold_in(splits[7], 1), -9, (-4) - 1).astype(jnp.int32)
    output_blocks = gaussian(splits[8], (HEADS * HEAD_DIM // BLOCK, BLOCK, D), 1.0, 6.0, ((0, 4), (2, 64)))
    output_scales = set_ends(jax.random.randint(splits[9], (HEADS * HEAD_DIM // BLOCK, 1, D), -9, -4), jax.random.fold_in(splits[9], 1), -9, (-4) - 1).astype(jnp.int32)
    return dict(activations=activations, norm_gain=norm_gain, query_blocks=query_blocks, query_scales=query_scales, key_blocks=key_blocks, key_scales=key_scales, value_blocks=value_blocks, value_scales=value_scales, output_blocks=output_blocks, output_scales=output_scales)


EPS = 1e-05
ROPE_BASE = 500000.0

def dequant(blocks, scales):
    factor = jnp.exp2(scales.astype(jnp.float32)).astype(blocks.dtype)
    weight = blocks * factor
    return weight.reshape(weight.shape[0] * weight.shape[1], weight.shape[2])

def rotate_pairs(states, positions):
    half_dim = states.shape[-1] // 2
    frequency = jnp.exp(-math.log(ROPE_BASE) * jnp.arange(half_dim, dtype=jnp.float32) * 2.0 / states.shape[-1])
    angles = positions.astype(jnp.float32)[:, None] * frequency[None, :]
    cosine = jnp.cos(angles)[None, :, None, :]
    sine_part = jnp.sin(angles)[None, :, None, :]
    first = states[..., :half_dim]
    second = states[..., half_dim:]
    return jnp.concatenate([first * cosine - second * sine_part, second * cosine + first * sine_part], axis=-1)

def attend(query_states, key_states, value_states, kv_count):
    tokens_here = query_states.shape[0]
    count = tokens_here // SEQ
    positions = jnp.arange(SEQ, dtype=jnp.int32)
    queries = rotate_pairs(query_states.reshape(count, SEQ, -1, HEAD_DIM), positions).astype(jnp.bfloat16)
    rotated_keys = rotate_pairs(key_states.reshape(count, SEQ, kv_count, HEAD_DIM), positions).astype(jnp.bfloat16)
    value_heads = value_states.astype(jnp.bfloat16).reshape(count, SEQ, kv_count, HEAD_DIM)
    group_size = queries.shape[2] // kv_count
    queries = queries.reshape(count, SEQ, kv_count, group_size, HEAD_DIM)
    scores = jnp.einsum('sqkgd,stkd->skgqt', queries.astype(jnp.float32), rotated_keys.astype(jnp.float32)) * HEAD_DIM ** (-0.5)
    visible = positions[:, None] >= positions[None, :]
    scores = jnp.where(visible, scores, -jnp.inf)
    attn_weights = jax.nn.softmax(scores, axis=-1).astype(jnp.bfloat16)
    context = jnp.einsum('skgqt,stkd->sqkgd', attn_weights.astype(jnp.float32), value_heads.astype(jnp.float32))
    return context.astype(jnp.bfloat16).reshape(tokens_here, -1)

def reference(activations, norm_gain, query_blocks, query_scales, key_blocks, key_scales, value_blocks, value_scales, output_blocks, output_scales):
    query_weight = dequant(query_blocks, query_scales)
    key_weight = dequant(key_blocks, key_scales)
    value_weight = dequant(value_blocks, value_scales)
    output_weight = dequant(output_blocks, output_scales)
    group_rows = SEQS * SEQ
    share = HEADS * HEAD_DIM // N_TENSOR
    kv_share = KV_HEADS * HEAD_DIM // N_TENSOR
    grouped = activations.reshape(N_DP, group_rows, D)

    def one_group(rows):
        wide_rows = rows.astype(jnp.float32)
        inverse = lax.rsqrt(lax.optimization_barrier(jnp.mean(wide_rows * wide_rows, axis=-1, keepdims=True)) + EPS)
        normed = (wide_rows * inverse * norm_gain.astype(jnp.float32)).astype(jnp.bfloat16)
        summed = jnp.zeros((group_rows, D), jnp.float32)
        for member in range(N_TENSOR):
            query_states = jnp.dot(normed, query_weight[:, member * share:(member + 1) * share], preferred_element_type=jnp.float32)
            key_states = jnp.dot(normed, key_weight[:, member * kv_share:(member + 1) * kv_share], preferred_element_type=jnp.float32)
            value_states = jnp.dot(normed, value_weight[:, member * kv_share:(member + 1) * kv_share], preferred_element_type=jnp.float32)
            context = attend(query_states, key_states, value_states, KV_HEADS // N_TENSOR)
            partial_value = jnp.dot(context, output_weight[member * share:(member + 1) * share], preferred_element_type=jnp.float32).astype(jnp.bfloat16)
            partial_value = lax.optimization_barrier(partial_value)
            summed = summed + partial_value.astype(jnp.float32)
        return summed.astype(jnp.bfloat16)
    return lax.map(one_group, grouped).reshape(TOKENS, D)
```

```python
import functools
import math

import jax
import jax.numpy as jnp
from jax import lax
from jax.experimental import pallas as pl
from jax.experimental.pallas import tpu as pltpu
from jax.sharding import PartitionSpec as P

HEAD_DIM = 128
SEQ = 256
EPS = 1e-05
ROPE_BASE = 500000.0
MESH = pl.DeviceIdType.MESH
OFF = (0, -1, 1, 2)
LAG = 3
ROWS = 64


def turn(v, d):
    return lax.rem(v + (d + 4), 4)


class Half:
    def __init__(self, half, own, buf, recv, send, place):
        self.half, self.own, self.buf, self.recv, self.sent = half, own, buf, recv, send
        x, y, z = place
        self.z = z
        self.m, self.l = (x, y) if half == 0 else (y, x)
        self.waited = {(0, 0, 0)}

    def index(self, m, l, z):
        return l * 16 + z * 4 + m if self.half == 0 else m * 16 + z * 4 + l

    def slot(self, key):
        r, jm, jl = key
        return self.index(turn(self.m, OFF[jm]), turn(self.l, OFF[jl]), turn(self.z, OFF[r]))

    def rows(self, key):
        return self.buf.at[pl.ds(pl.multiple_of(self.slot(key) * ROWS, ROWS), ROWS)]

    def copy(self, key, device):
        src = self.own if key == (0, 0, 0) else self.rows(key)
        return pltpu.make_async_remote_copy(
            src_ref=src,
            dst_ref=self.rows(key),
            send_sem=self.sent,
            recv_sem=self.recv.at[self.slot(key)],
            device_id={"dp": device},
            device_id_type=MESH,
        )

    def near(self, dim, d):
        m, l, z = self.m, self.l, self.z
        if dim == "z":
            z = turn(z, d)
        elif dim == "m":
            m = turn(m, d)
        else:
            l = turn(l, d)
        return self.index(m, l, z)

    def ensure(self, key):
        if key not in self.waited:
            self.waited.add(key)
            self.copy(key, self.near("m", 1)).wait_recv()

    def both(self, key, dim):
        self.ensure(key)
        self.copy(key, self.near(dim, 1)).start()
        self.copy(key, self.near(dim, -1)).start()

    def forward(self, key_minus, key_plus, dim, way):
        if way % 2 == 0:
            self.ensure(key_minus)
            self.copy(key_minus, self.near(dim, 1)).start()
        else:
            self.ensure(key_plus)
            self.copy(key_plus, self.near(dim, -1)).start()

    def zed(self):
        self.both((0, 0, 0), "z")

    def zed_on(self):
        self.forward((1, 0, 0), (2, 0, 0), "z", self.half)

    def mid(self, r):
        self.both((r, 0, 0), "m")

    def mid_on(self, r):
        self.forward((r, 1, 0), (r, 2, 0), "m", r)

    def last(self, r, j):
        self.both((r, j, 0), "l")

    def last_on(self, r, j):
        self.forward((r, j, 1), (r, j, 2), "l", j)

    def done(self, r):
        for j in range(4):
            for k in range(4):
                self.ensure((r, j, k))

    def drain(self):
        part = self.buf.at[pl.ds(0, 63 * ROWS)]
        pltpu.make_async_remote_copy(
            src_ref=part,
            dst_ref=part,
            send_sem=self.sent,
            recv_sem=self.recv.at[0],
            device_id={"dp": self.near("m", 1)},
            device_id_type=MESH,
        ).wait_send()


def gather_kernel(qa_in, qb_in, oa_in, ob_in, qa, qb, oa, ob, recv, sent):
    dp = lax.axis_index("dp")
    x, z, y = lax.rem(dp, 4), lax.rem(dp // 4, 4), dp // 16
    place = (x, y, z)
    refs = (((qa_in, qa), (qb_in, qb)), ((oa_in, oa), (ob_in, ob)))
    streams = [
        [Half(h, *refs[s][h], recv.at[s, h], sent.at[s, h], place) for h in range(2)]
        for s in range(2)
    ]
    first = streams[0][0]
    barrier = pltpu.get_barrier_semaphore()
    for dim in ("m", "l", "z"):
        for d in (1, -1):
            pl.semaphore_signal(
                barrier, inc=1, device_id={"dp": first.near(dim, d)}, device_id_type=MESH
            )
    pl.semaphore_wait(barrier, 6)
    for st in streams[0]:
        st.last(0, 0)
        st.mid(0)
        st.zed()
    for st in streams[0]:
        st.mid_on(0)
        st.zed_on()
    for s in range(2):
        for st in streams[s]:
            slot = pl.ds(pl.multiple_of(dp * ROWS, ROWS), ROWS)
            st.buf[slot, :] = st.own[...]

    def on(i):
        for st in streams[i // 16]:
            st.last_on((i // 4) % 4, i % 4)

    for i in range(32):
        s, r, j = i // 16, (i // 4) % 4, i % 4
        if i > 0:
            for st in streams[s]:
                st.last(r, j)
        n = i // 4 + 1
        if n < 8:
            if j == 0:
                for st in streams[n // 4]:
                    st.mid(n % 4)
            if j == 2:
                for st in streams[n // 4]:
                    st.mid_on(n % 4)
        if i == 8:
            for st in streams[1]:
                st.zed()
        if i == 10:
            for st in streams[1]:
                st.zed_on()
        if i >= LAG:
            on(i - LAG)
    for i in range(32 - LAG, 32):
        on(i)
    for s in range(2):
        for st in streams[s]:
            for r in range(4):
                st.done(r)
    for s in range(2):
        for st in streams[s]:
            st.drain()


def gather(qa, qb, oa, ob):
    vmem = pl.BlockSpec(memory_space=pltpu.VMEM)
    whole = [jax.ShapeDtypeStruct((64 * ROWS, a.shape[1]), a.dtype) for a in (qa, qb, oa, ob)]
    return pl.pallas_call(
        gather_kernel,
        out_shape=whole,
        in_specs=[vmem] * 4,
        out_specs=[vmem] * 4,
        scratch_shapes=[
            pltpu.SemaphoreType.DMA((2, 2, 64)),
            pltpu.SemaphoreType.DMA((2, 2)),
        ],
        compiler_params=pltpu.CompilerParams(
            collective_id=0, has_side_effects=True, vmem_limit_bytes=60 * 2**20
        ),
    )(qa, qb, oa, ob)


def dequant(blocks, scales):
    factor = jnp.exp2(scales.astype(jnp.float32)).astype(blocks.dtype)
    weight = blocks * factor
    return weight.reshape(weight.shape[0] * weight.shape[1], weight.shape[2])


def rotate_pairs(states, positions):
    half_dim = states.shape[-1] // 2
    frequency = jnp.exp(
        -math.log(ROPE_BASE) * jnp.arange(half_dim, dtype=jnp.float32) * 2.0 / states.shape[-1]
    )
    angles = positions.astype(jnp.float32)[:, None] * frequency[None, :]
    cosine = jnp.cos(angles)[None, :, None, :]
    sine_part = jnp.sin(angles)[None, :, None, :]
    first = states[..., :half_dim]
    second = states[..., half_dim:]
    return jnp.concatenate(
        [first * cosine - second * sine_part, second * cosine + first * sine_part], axis=-1
    )


def attend(query_states, key_states, value_states, kv_count):
    tokens_here = query_states.shape[0]
    count = tokens_here // SEQ
    positions = jnp.arange(SEQ, dtype=jnp.int32)
    queries = rotate_pairs(query_states.reshape(count, SEQ, -1, HEAD_DIM), positions).astype(
        jnp.bfloat16
    )
    rotated_keys = rotate_pairs(
        key_states.reshape(count, SEQ, kv_count, HEAD_DIM), positions
    ).astype(jnp.bfloat16)
    value_heads = value_states.astype(jnp.bfloat16).reshape(count, SEQ, kv_count, HEAD_DIM)
    group_size = queries.shape[2] // kv_count
    queries = queries.reshape(count, SEQ, kv_count, group_size, HEAD_DIM)
    scores = jnp.einsum(
        "sqkgd,stkd->skgqt", queries, rotated_keys, preferred_element_type=jnp.float32
    ) * HEAD_DIM ** (-0.5)
    visible = positions[:, None] >= positions[None, :]
    scores = jnp.where(visible, scores, -jnp.inf)
    attn_weights = jax.nn.softmax(scores, axis=-1).astype(jnp.bfloat16)
    context = jnp.einsum(
        "skgqt,stkd->sqkgd", attn_weights, value_heads, preferred_element_type=jnp.float32
    )
    return context.astype(jnp.bfloat16).reshape(tokens_here, -1)


def shards(
    activations,
    norm_gain,
    query_blocks,
    query_scales,
    key_blocks,
    key_scales,
    value_blocks,
    value_scales,
    output_blocks,
    output_scales,
):
    query = dequant(query_blocks, query_scales)
    key = dequant(key_blocks, key_scales)
    value = dequant(value_blocks, value_scales)
    output = dequant(output_blocks, output_scales).T
    qa_in = jnp.concatenate([query[:, :512], key], axis=1)
    qb_in = jnp.concatenate([query[:, 512:], value], axis=1)
    qa, qb, oa, ob = gather(qa_in, qb_in, output[:, :512], output[:, 512:])
    wide_rows = activations.astype(jnp.float32)
    inverse = lax.rsqrt(jnp.mean(wide_rows * wide_rows, axis=-1, keepdims=True) + EPS)
    normed = (wide_rows * inverse * norm_gain.astype(jnp.float32)).astype(jnp.bfloat16)
    a = jnp.dot(normed, qa, preferred_element_type=jnp.float32)
    b = jnp.dot(normed, qb, preferred_element_type=jnp.float32)
    query_states = jnp.concatenate([a[:, :512], b[:, :512]], axis=1)
    context = attend(query_states, a[:, 512:], b[:, 512:], 1)
    partial_value = lax.dot_general(
        context[:, :512], oa, (((1,), (1,)), ((), ())), preferred_element_type=jnp.float32
    ) + lax.dot_general(
        context[:, 512:], ob, (((1,), (1,)), ((), ())), preferred_element_type=jnp.float32
    )
    return lax.psum(partial_value.astype(jnp.bfloat16), "tensor")


def solution(mesh):
    placed = (
        P("dp", None),
        P(),
        P("dp", None, "tensor"),
        P("dp", None, "tensor"),
        P("dp", None, "tensor"),
        P("dp", None, "tensor"),
        P("dp", None, "tensor"),
        P("dp", None, "tensor"),
        P("tensor", None, "dp"),
        P("tensor", None, "dp"),
    )
    return jax.shard_map(
        shards, mesh=mesh, in_specs=placed, out_specs=P("dp", None), check_vma=False
    )
```

```python
import math

import jax
import jax.numpy as jnp
import numpy as np
from jax import lax
from jax.experimental import pallas as pl
from jax.experimental.pallas import tpu as pltpu
from jax.sharding import PartitionSpec as P

HEAD_DIM = 128
SEQ = 256
EPS = 1e-05
ROPE_BASE = 500000.0
MESH = pl.DeviceIdType.MESH
OFF = (0, -1, 1, 2)
LAG = 3
ROWS = 64


def turn(v, d):
    return lax.rem(v + (d + 4), 4)


class Half:
    def __init__(self, half, buf, recv, send, place):
        self.half, self.buf, self.recv, self.sent = half, buf, recv, send
        x, y, z = place
        self.z = z
        self.m, self.l = (x, y) if half == 0 else (y, x)
        self.waited = {(0, 0, 0)}

    def index(self, m, l, z):
        return l * 16 + z * 4 + m if self.half == 0 else m * 16 + z * 4 + l

    def slot(self, key):
        r, jm, jl = key
        return self.index(turn(self.m, OFF[jm]), turn(self.l, OFF[jl]), turn(self.z, OFF[r]))

    def rows(self, key):
        return self.buf.at[pl.ds(pl.multiple_of(self.slot(key) * ROWS, ROWS), ROWS)]

    def copy(self, key, device):
        return pltpu.make_async_remote_copy(
            src_ref=self.rows(key),
            dst_ref=self.rows(key),
            send_sem=self.sent,
            recv_sem=self.recv.at[self.slot(key)],
            device_id={"dp": device},
            device_id_type=MESH,
        )

    def near(self, dim, d):
        m, l, z = self.m, self.l, self.z
        if dim == "z":
            z = turn(z, d)
        elif dim == "m":
            m = turn(m, d)
        else:
            l = turn(l, d)
        return self.index(m, l, z)

    def ensure(self, key):
        if key not in self.waited:
            self.waited.add(key)
            self.copy(key, self.near("m", 1)).wait_recv()

    def both(self, key, dim):
        self.ensure(key)
        self.copy(key, self.near(dim, 1)).start()
        self.copy(key, self.near(dim, -1)).start()

    def forward(self, key_minus, key_plus, dim, way):
        if way % 2 == 0:
            self.ensure(key_minus)
            self.copy(key_minus, self.near(dim, 1)).start()
        else:
            self.ensure(key_plus)
            self.copy(key_plus, self.near(dim, -1)).start()

    def zed(self):
        self.both((0, 0, 0), "z")

    def zed_on(self):
        self.forward((1, 0, 0), (2, 0, 0), "z", self.half)

    def mid(self, r):
        self.both((r, 0, 0), "m")

    def mid_on(self, r):
        self.forward((r, 1, 0), (r, 2, 0), "m", r)

    def last(self, r, j):
        self.both((r, j, 0), "l")

    def last_on(self, r, j):
        self.forward((r, j, 1), (r, j, 2), "l", j)

    def done(self, r):
        for j in range(4):
            for k in range(4):
                self.ensure((r, j, k))

    def drain(self):
        part = self.buf.at[pl.ds(0, 63 * ROWS)]
        pltpu.make_async_remote_copy(
            src_ref=part,
            dst_ref=part,
            send_sem=self.sent,
            recv_sem=self.recv.at[0],
            device_id={"dp": self.near("m", 1)},
            device_id_type=MESH,
        ).wait_send()


def product(a, b):
    return jnp.dot(a, b, preferred_element_type=jnp.float32)


def product_t(a, b):
    return lax.dot_general(a, b, (((1,), (1,)), ((), ())), preferred_element_type=jnp.float32)


def layer_kernel(
    act_in,
    gain,
    cosine,
    sine,
    qa_in,
    qb_in,
    oa_in,
    ob_in,
    out,
    act,
    qa,
    qb,
    oa,
    ob,
    acc_a,
    acc_b,
    keys,
    values,
    context,
    give,
    keep,
    got,
    pair,
    over,
    total,
    recv,
    sent,
    sum_recv,
    sum_sent,
    io,
):
    dp = lax.axis_index("dp")
    tensor = lax.axis_index("tensor")
    x, z, y = lax.rem(dp, 4), lax.rem(dp // 4, 4), dp // 16
    core = lax.rem(tensor, 2)
    sibling = tensor + 1 - 2 * core
    partner = lax.rem(tensor + 2, 4)
    mine = pl.ds(pl.multiple_of(core * SEQ, SEQ), SEQ)
    other = pl.ds(pl.multiple_of((1 - core) * SEQ, SEQ), SEQ)
    slot = pl.ds(pl.multiple_of(dp * ROWS, ROWS), ROWS)
    bufs = ((qa, qb), (oa, ob))
    streams = [
        [Half(h, bufs[s][h], recv.at[s, h], sent.at[s, h], (x, y, z)) for h in range(2)]
        for s in range(2)
    ]
    first = streams[0][0]
    loads = [
        pltpu.make_async_copy(src, dst.at[slot], io.at[k])
        for k, (src, dst) in enumerate(((qa_in, qa), (qb_in, qb), (oa_in, oa), (ob_in, ob)))
    ]
    load_act = pltpu.make_async_copy(act_in, act, io.at[4])
    for load in loads:
        load.start()
    load_act.start()
    barrier = pltpu.get_barrier_semaphore()
    for dim in ("m", "l", "z"):
        for d in (1, -1):
            pl.semaphore_signal(
                barrier, inc=1, device_id={"dp": first.near(dim, d)}, device_id_type=MESH
            )
    for peer in (sibling, partner):
        pl.semaphore_signal(barrier, inc=1, device_id={"tensor": peer}, device_id_type=MESH)
    pl.semaphore_wait(barrier, 8)
    loads[0].wait()
    loads[1].wait()
    for st in streams[0]:
        st.last(0, 0)
        st.mid(0)
        st.zed()
    for st in streams[0]:
        st.mid_on(0)
        st.zed_on()
    loads[2].wait()
    loads[3].wait()
    acc_a[...] = jnp.zeros_like(acc_a)
    acc_b[...] = jnp.zeros_like(acc_b)
    load_act.wait()

    def norm(k):
        @pl.loop(0, 8)
        def _(i):
            rows = pl.ds(pl.multiple_of(k * 128 + i * 16, 16), 16)
            wide = act[rows, :].astype(jnp.float32)
            mean = jnp.mean(wide * wide, axis=-1, keepdims=True)
            scaled = wide * lax.rsqrt(mean + EPS) * gain[...].astype(jnp.float32)
            act[rows, :] = scaled.astype(jnp.bfloat16)

    def project(r):
        for st in streams[0]:
            st.done(r)
        zs = turn(z, OFF[r])

        @pl.loop(0, 4)
        def _(k):
            part = pl.ds(pl.multiple_of((k * 4 + zs) * 256, 256), 256)
            acc_a[...] += product(act[:, part], qa[part, :])
            acc_b[...] += product(act[:, part], qb[part, :])

    def rotate(states):
        return states * cosine[...] + pltpu.roll(states, HEAD_DIM // 2, 1) * sine[...]

    def keys_values(s):
        rows = pl.ds(s * SEQ, SEQ)
        keys[rows, :] = rotate(acc_a[rows, 512:]).astype(jnp.bfloat16)
        values[rows, :] = acc_b[rows, 512:].astype(jnp.bfloat16)

    def attend(s, h):
        rows = pl.ds(s * SEQ, SEQ)
        acc = (acc_a, acc_b)[h]

        @pl.loop(0, 4)
        def _(k):
            head = pl.ds(pl.multiple_of(k * HEAD_DIM, HEAD_DIM), HEAD_DIM)
            queries = rotate(acc[rows, head]).astype(jnp.bfloat16)
            scores = product_t(queries, keys[rows, :]) * HEAD_DIM ** (-0.5)
            spot = lax.broadcasted_iota(jnp.int32, (SEQ, SEQ), 0)
            seen = lax.broadcasted_iota(jnp.int32, (SEQ, SEQ), 1)
            scores = jnp.where(spot >= seen, scores, -jnp.inf)
            raised = jnp.exp(scores - jnp.max(scores, axis=-1, keepdims=True))
            weights = raised * (1.0 / jnp.sum(raised, axis=-1, keepdims=True))
            wide = product(weights.astype(jnp.bfloat16), values[rows, :])
            place = pl.ds(pl.multiple_of(h * 512 + k * HEAD_DIM, HEAD_DIM), HEAD_DIM)
            context[rows, place] = wide.astype(jnp.bfloat16)

    def block(n):
        return lax.rem(n, 4) * 4 + turn(z, OFF[n // 4])

    def tensor_copy(stage, n, src, dst, peer):
        c = block(n)
        return pltpu.make_async_remote_copy(
            src_ref=src,
            dst_ref=dst,
            send_sem=sum_sent.at[stage],
            recv_sem=sum_recv.at[stage, c],
            device_id={"tensor": peer},
            device_id_type=MESH,
        )

    def hand(n):
        c = block(n)
        return tensor_copy(0, n, give.at[c], got.at[c], sibling)

    def cross(n):
        c = block(n)
        return tensor_copy(1, n, pair.at[c], over.at[c], partner)

    def share(n):
        c = block(n)
        return tensor_copy(2, n, total.at[c, mine], total.at[c, mine], sibling)

    def share_in(n):
        c = block(n)
        return tensor_copy(2, n, total.at[c, other], total.at[c, other], sibling)

    def put(n, half):
        c = block(n)
        columns = pl.ds(pl.multiple_of(c * 256, 256), 256)
        return pltpu.make_async_copy(total.at[c, half], out.at[half, columns], io.at[5])

    def partial(n, rows):
        part = pl.ds(pl.multiple_of(block(n) * 256, 256), 256)
        wide = product_t(context[rows, :512], oa[part, :]) + product_t(
            context[rows, 512:], ob[part, :]
        )
        return wide.astype(jnp.bfloat16)

    def pairs(n):
        c = block(n)
        hand(n).wait_recv()
        wide = keep[c].astype(jnp.float32) + got[c].astype(jnp.float32)
        pair[c] = wide.astype(jnp.bfloat16)

    def totals(n):
        c = block(n)
        cross(n).wait_recv()
        wide = pair[c].astype(jnp.float32) + over[c].astype(jnp.float32)
        total[c, mine, :] = wide.astype(jnp.bfloat16)

    def step(n):
        if n < 16 and n % 4 == 0:
            for st in streams[1]:
                st.done(n // 4)
        two, three, four = n - 1, n - 3, n - 4
        if 0 <= two < 16:
            pairs(two)
        if 0 <= three < 16:
            totals(three)
        if n < 16:
            give[block(n)] = partial(n, other)
        if 0 <= two < 16:
            cross(two).start()
        if 0 <= three < 16:
            share(three).start()
            put(three, mine).start()
        if 0 <= four < 16:
            share_in(four).wait_recv()
            put(four, other).start()
        if n < 16:
            keep[block(n)] = partial(n, mine)
            hand(n).start()

    def on(i):
        for st in streams[i // 16]:
            st.last_on((i // 4) % 4, i % 4)

    work = {i: [lambda k=i: norm(k)] for i in range(4)}
    for r in range(3):
        work.setdefault(4 * r + 7, []).append(lambda k=r: project(k))
    work[18] = [lambda: project(3), lambda: keys_values(0), lambda: keys_values(1)]
    work[19] = [lambda: attend(0, 0), lambda: attend(0, 1)]
    work[20] = [lambda: attend(1, 0), lambda: attend(1, 1)]
    for n, o in enumerate((6, 6, 7, 8, 10, 11, 12, 13, 14, 15)):
        work.setdefault(16 + o, []).append(lambda k=n: step(k))

    for i in range(32):
        s, r, j = i // 16, (i // 4) % 4, i % 4
        if i > 0:
            for st in streams[s]:
                st.last(r, j)
        n = i // 4 + 1
        if n < 8:
            if j == 0:
                for st in streams[n // 4]:
                    st.mid(n % 4)
            if j == 2:
                for st in streams[n // 4]:
                    st.mid_on(n % 4)
        if i == 8:
            for st in streams[1]:
                st.zed()
        if i == 10:
            for st in streams[1]:
                st.zed_on()
        if i >= LAG:
            on(i - LAG)
        for task in work.get(i, ()):
            task()
    for i in range(32 - LAG, 32):
        on(i)
    for n in range(10, 20):
        step(n)
    for s in range(2):
        for st in streams[s]:
            st.drain()
    for stage, ref in enumerate((give, pair, total.at[:, :SEQ])):
        pltpu.make_async_remote_copy(
            src_ref=ref,
            dst_ref=ref,
            send_sem=sum_sent.at[stage],
            recv_sem=sum_recv.at[stage, 0],
            device_id={"tensor": sibling},
            device_id_type=MESH,
        ).wait_send()
    pltpu.make_async_copy(out, out, io.at[5]).wait()


def tables():
    half = HEAD_DIM // 2
    frequency = np.exp(-math.log(ROPE_BASE) * np.arange(half) * 2.0 / HEAD_DIM)
    angles = np.arange(SEQ)[:, None] * frequency[None, :]
    cosine, sine = np.cos(angles), np.sin(angles)
    return (
        np.concatenate([cosine, cosine], axis=1).astype(np.float32),
        np.concatenate([-sine, sine], axis=1).astype(np.float32),
    )


def layer(activations, gain, qa, qb, oa, ob):
    vmem = pl.BlockSpec(memory_space=pltpu.VMEM)
    hbm = pl.BlockSpec(memory_space=pltpu.HBM)
    tokens, features = activations.shape
    cosine, sine = tables()
    kind = jnp.bfloat16
    chunks = features // 256
    return pl.pallas_call(
        layer_kernel,
        out_shape=jax.ShapeDtypeStruct((tokens, features), kind),
        in_specs=[hbm, vmem, vmem, vmem, hbm, hbm, hbm, hbm],
        out_specs=hbm,
        scratch_shapes=[
            pltpu.VMEM((tokens, features), kind),
            pltpu.VMEM((features, 640), kind),
            pltpu.VMEM((features, 640), kind),
            pltpu.VMEM((features, 512), kind),
            pltpu.VMEM((features, 512), kind),
            pltpu.VMEM((tokens, 640), jnp.float32),
            pltpu.VMEM((tokens, 640), jnp.float32),
            pltpu.VMEM((tokens, HEAD_DIM), kind),
            pltpu.VMEM((tokens, HEAD_DIM), kind),
            pltpu.VMEM((tokens, 1024), kind),
            pltpu.VMEM((chunks, SEQ, 256), kind),
            pltpu.VMEM((chunks, SEQ, 256), kind),
            pltpu.VMEM((chunks, SEQ, 256), kind),
            pltpu.VMEM((chunks, SEQ, 256), kind),
            pltpu.VMEM((chunks, SEQ, 256), kind),
            pltpu.VMEM((chunks, tokens, 256), kind),
            pltpu.SemaphoreType.DMA((2, 2, 64)),
            pltpu.SemaphoreType.DMA((2, 2)),
            pltpu.SemaphoreType.DMA((3, 16)),
            pltpu.SemaphoreType.DMA((3,)),
            pltpu.SemaphoreType.DMA((6,)),
        ],
        compiler_params=pltpu.CompilerParams(
            collective_id=0, has_side_effects=True, vmem_limit_bytes=60 * 2**20
        ),
    )(activations, gain, cosine, sine, qa, qb, oa, ob)


def dequant(blocks, scales):
    factor = jnp.exp2(scales.astype(jnp.float32)).astype(blocks.dtype)
    weight = blocks * factor
    return weight.reshape(weight.shape[0] * weight.shape[1], weight.shape[2])


def shards(
    activations,
    norm_gain,
    query_blocks,
    query_scales,
    key_blocks,
    key_scales,
    value_blocks,
    value_scales,
    output_blocks,
    output_scales,
):
    query = dequant(query_blocks, query_scales)
    key = dequant(key_blocks, key_scales)
    value = dequant(value_blocks, value_scales)
    output = dequant(output_blocks, output_scales).T
    qa = jnp.concatenate([query[:, :512], key], axis=1)
    qb = jnp.concatenate([query[:, 512:], value], axis=1)
    return layer(
        activations, norm_gain.reshape(1, -1), qa, qb, output[:, :512], output[:, 512:]
    )


def solution(mesh):
    placed = (
        P("dp", None),
        P(),
        P("dp", None, "tensor"),
        P("dp", None, "tensor"),
        P("dp", None, "tensor"),
        P("dp", None, "tensor"),
        P("dp", None, "tensor"),
        P("dp", None, "tensor"),
        P("tensor", None, "dp"),
        P("tensor", None, "dp"),
    )
    return jax.shard_map(
        shards, mesh=mesh, in_specs=placed, out_specs=P("dp", None), check_vma=False
    )
```

```python
import math

import jax
import jax.numpy as jnp
import numpy as np
from jax import lax
from jax.experimental import pallas as pl
from jax.experimental.pallas import tpu as pltpu
from jax.sharding import PartitionSpec as P

HEAD_DIM = 128
SEQ = 256
EPS = 1e-05
ROPE_BASE = 500000.0
MESH = pl.DeviceIdType.MESH
OFF = (0, -1, 1, 2)
ROWS = 64


def turn(v, d):
    return lax.rem(v + (d + 4), 4)


class Half:
    def __init__(self, half, buf, recv, send, place):
        self.half, self.buf, self.recv, self.sent = half, buf, recv, send
        x, y, z = place
        self.z = z
        self.m, self.l = (x, y) if half == 0 else (y, x)
        self.waited = {(0, 0, 0)}

    def index(self, m, l, z):
        return l * 16 + z * 4 + m if self.half == 0 else m * 16 + z * 4 + l

    def slot(self, key):
        r, jm, jl = key
        return self.index(turn(self.m, OFF[jm]), turn(self.l, OFF[jl]), turn(self.z, OFF[r]))

    def rows(self, key):
        return self.buf.at[pl.ds(pl.multiple_of(self.slot(key) * ROWS, ROWS), ROWS)]

    def copy(self, key, device):
        return pltpu.make_async_remote_copy(
            src_ref=self.rows(key),
            dst_ref=self.rows(key),
            send_sem=self.sent,
            recv_sem=self.recv.at[self.slot(key)],
            device_id={"dp": device},
            device_id_type=MESH,
        )

    def near(self, dim, d):
        m, l, z = self.m, self.l, self.z
        if dim == "z":
            z = turn(z, d)
        elif dim == "m":
            m = turn(m, d)
        else:
            l = turn(l, d)
        return self.index(m, l, z)

    def ensure(self, key):
        if key not in self.waited:
            self.waited.add(key)
            self.copy(key, self.near("m", 1)).wait_recv()

    def both(self, key, dim):
        self.ensure(key)
        self.copy(key, self.near(dim, 1)).start()
        self.copy(key, self.near(dim, -1)).start()

    def forward(self, key_minus, key_plus, dim, way):
        if way % 2 == 0:
            self.ensure(key_minus)
            self.copy(key_minus, self.near(dim, 1)).start()
        else:
            self.ensure(key_plus)
            self.copy(key_plus, self.near(dim, -1)).start()

    def zed(self):
        self.both((0, 0, 0), "z")

    def zed_on(self):
        self.forward((1, 0, 0), (2, 0, 0), "z", self.half)

    def mid(self, r):
        self.both((r, 0, 0), "m")

    def mid_on(self, r):
        self.forward((r, 1, 0), (r, 2, 0), "m", r)

    def last(self, r, j):
        self.both((r, j, 0), "l")

    def last_on(self, r, j):
        self.forward((r, j, 1), (r, j, 2), "l", j)

    def drain(self):
        part = self.buf.at[pl.ds(0, 63 * ROWS)]
        pltpu.make_async_remote_copy(
            src_ref=part,
            dst_ref=part,
            send_sem=self.sent,
            recv_sem=self.recv.at[0],
            device_id={"dp": self.near("m", 1)},
            device_id_type=MESH,
        ).wait_send()


def product(a, b):
    return jnp.dot(a, b, preferred_element_type=jnp.float32)


def product_t(a, b):
    return lax.dot_general(a, b, (((1,), (1,)), ((), ())), preferred_element_type=jnp.float32)


def layer_kernel(
    act_in,
    gain,
    cosine,
    sine,
    query_in,
    query_exp,
    key_in,
    key_exp,
    value_in,
    value_exp,
    output_in,
    output_exp,
    out,
    act,
    qa,
    qb,
    oa,
    ob,
    acc_a,
    acc_b,
    keys,
    values,
    context,
    give,
    keep,
    got,
    pair,
    over,
    total,
    gain_row,
    flat,
    recv,
    sent,
    sum_recv,
    sum_sent,
    io,
):
    dp = lax.axis_index("dp")
    tensor = lax.axis_index("tensor")
    x, z, y = lax.rem(dp, 4), lax.rem(dp // 4, 4), dp // 16
    core = lax.rem(tensor, 2)
    sibling = tensor + 1 - 2 * core
    partner = lax.rem(tensor + 2, 4)
    mine = pl.ds(pl.multiple_of(core * SEQ, SEQ), SEQ)
    other = pl.ds(pl.multiple_of((1 - core) * SEQ, SEQ), SEQ)
    bufs = ((qa, qb), (oa, ob))
    streams = [
        [Half(h, bufs[s][h], recv.at[s, h], sent.at[s, h], (x, y, z)) for h in range(2)]
        for s in range(2)
    ]
    first = streams[0][0]
    load_act = pltpu.make_async_copy(act_in, act, io.at[0])
    load_act.start()
    barrier = pltpu.get_barrier_semaphore()
    for dim in ("m", "l", "z"):
        for d in (1, -1):
            pl.semaphore_signal(
                barrier, inc=1, device_id={"dp": first.near(dim, d)}, device_id_type=MESH
            )
    for peer in (sibling, partner):
        pl.semaphore_signal(barrier, inc=1, device_id={"tensor": peer}, device_id_type=MESH)

    def factor(exponents):
        return jnp.exp2(exponents.astype(jnp.float32)).astype(jnp.bfloat16)

    for b in range(2):
        rows = pl.ds(pl.multiple_of(dp * ROWS + b * 32, 32), 32)
        query = query_in[b] * factor(query_exp[b])
        qa[rows, :512] = query[:, :512]
        qb[rows, :512] = query[:, 512:]
        qa[rows, 512:] = key_in[b] * factor(key_exp[b])
        qb[rows, 512:] = value_in[b] * factor(value_exp[b])

    def fill_output():
        for b in range(32):
            flat[b * 32 : (b + 1) * 32, :] = output_in[b] * factor(output_exp[b])
        rows = pl.ds(pl.multiple_of(dp * ROWS, ROWS), ROWS)
        oa[rows, :] = flat[:512, :].T
        ob[rows, :] = flat[512:, :].T

    def fill_gain():
        for k in range(32):
            gain_row[:, k * 128 : (k + 1) * 128] = gain[k : k + 1, :].astype(jnp.float32)
        acc_a[...] = jnp.zeros_like(acc_a)
        acc_b[...] = jnp.zeros_like(acc_b)

    pl.semaphore_wait(barrier, 8)

    def norm(k):
        @pl.loop(0, 8)
        def _(i):
            rows = pl.ds(pl.multiple_of(k * 128 + i * 16, 16), 16)
            wide = act[rows, :].astype(jnp.float32)
            mean = jnp.mean(wide * wide, axis=-1, keepdims=True)
            scaled = wide * lax.rsqrt(mean + EPS) * gain_row[...]
            act[rows, :] = scaled.astype(jnp.bfloat16)

    def need(s, r, k):
        for j in range(4):
            streams[s][0].ensure((r, j, k))
        for j in range(4):
            streams[s][1].ensure((r, k, j))

    def project(r, parts):
        for k in parts:
            need(0, r, k)
        zs = turn(z, OFF[r])

        @pl.loop(parts[0], parts[-1] + 1)
        def _(k):
            away = 3 * k + 3 * (k // 2) + 2 * (k // 3)
            spot = lax.rem(y + away, 4) * 4 + zs
            part = pl.ds(pl.multiple_of(spot * 256, 256), 256)
            acc_a[...] += product(act[:, part], qa[part, :])
            acc_b[...] += product(act[:, part], qb[part, :])

    def rotate(states):
        return states * cosine[...] + pltpu.roll(states, HEAD_DIM // 2, 1) * sine[...]

    def keys_values(s):
        rows = pl.ds(s * SEQ, SEQ)
        keys[rows, :] = rotate(acc_a[rows, 512:]).astype(jnp.bfloat16)
        values[rows, :] = acc_b[rows, 512:].astype(jnp.bfloat16)

    def attend(h):
        acc = (acc_a, acc_b)[h]

        @pl.loop(0, 2)
        def _(s):
            rows = pl.ds(pl.multiple_of(s * SEQ, SEQ), SEQ)
            spot = lax.broadcasted_iota(jnp.int32, (SEQ, SEQ), 0)
            seen = lax.broadcasted_iota(jnp.int32, (SEQ, SEQ), 1)
            for k in range(4):
                queries = rotate(acc[rows, k * HEAD_DIM : (k + 1) * HEAD_DIM])
                scores = product_t(queries.astype(jnp.bfloat16), keys[rows, :])
                scores = scores * HEAD_DIM ** (-0.5)
                scores = jnp.where(spot >= seen, scores, -jnp.inf)
                raised = jnp.exp(scores - jnp.max(scores, axis=-1, keepdims=True))
                weights = raised * (1.0 / jnp.sum(raised, axis=-1, keepdims=True))
                wide = product(weights.astype(jnp.bfloat16), values[rows, :])
                place = h * 512 + k * HEAD_DIM
                context[rows, place : place + HEAD_DIM] = wide.astype(jnp.bfloat16)

    def block(n):
        return turn(y, OFF[n % 4]) * 4 + turn(z, OFF[n // 4])

    def tensor_copy(stage, n, src, dst, peer):
        c = block(n)
        return pltpu.make_async_remote_copy(
            src_ref=src,
            dst_ref=dst,
            send_sem=sum_sent.at[stage],
            recv_sem=sum_recv.at[stage, c],
            device_id={"tensor": peer},
            device_id_type=MESH,
        )

    def hand(n):
        c = block(n)
        return tensor_copy(0, n, give.at[c], got.at[c], sibling)

    def cross(n):
        c = block(n)
        return tensor_copy(1, n, pair.at[c], over.at[c], partner)

    def share(n):
        c = block(n)
        return tensor_copy(2, n, total.at[c, mine], total.at[c, mine], sibling)

    def share_in(n):
        c = block(n)
        return tensor_copy(2, n, total.at[c, other], total.at[c, other], sibling)

    def put(n, half):
        c = block(n)
        columns = pl.ds(pl.multiple_of(c * 256, 256), 256)
        return pltpu.make_async_copy(total.at[c, half], out.at[half, columns], io.at[1])

    def partial(n, rows):
        part = pl.ds(pl.multiple_of(block(n) * 256, 256), 256)
        wide = product_t(context[rows, :512], oa[part, :]) + product_t(
            context[rows, 512:], ob[part, :]
        )
        return wide.astype(jnp.bfloat16)

    def pairs(n):
        c = block(n)
        hand(n).wait_recv()
        wide = keep[c].astype(jnp.float32) + got[c].astype(jnp.float32)
        pair[c] = wide.astype(jnp.bfloat16)

    def totals(n):
        c = block(n)
        cross(n).wait_recv()
        wide = pair[c].astype(jnp.float32) + over[c].astype(jnp.float32)
        total[c, mine, :] = wide.astype(jnp.bfloat16)

    def step(n):
        if n < 16:
            need(1, n // 4, n % 4)
        two, three, four = n - 1, n - 3, n - 4
        if 0 <= two < 16:
            pairs(two)
        if 0 <= three < 16:
            totals(three)
        if n < 16:
            give[block(n)] = partial(n, other)
        if 0 <= two < 16:
            cross(two).start()
        if 0 <= three < 16:
            share(three).start()
            put(three, mine).start()
        if 0 <= four < 16:
            share_in(four).wait_recv()
            put(four, other).start()
        if n < 16:
            keep[block(n)] = partial(n, mine)
            hand(n).start()

    def each(i, call):
        for st in streams[i]:
            call(st)

    def last(i):
        each(i // 16, lambda st: st.last((i // 4) % 4, i % 4))

    def on(i):
        each(i // 16, lambda st: st.last_on((i // 4) % 4, i % 4))

    def mid(q):
        each(q // 4, lambda st: st.mid(q % 4))

    def mid_on(q):
        each(q // 4, lambda st: st.mid_on(q % 4))

    def zed(s):
        each(s, lambda st: st.zed())

    def zed_on(s):
        each(s, lambda st: st.zed_on())

    mid(0), last(0), zed(0)
    fill_gain()
    load_act.wait()
    norm(0), norm(1)
    mid_on(0), last(1), last(2), on(0)
    norm(2)
    last(3), on(1), mid(1), zed_on(0)
    fill_output()
    norm(3)
    on(2), last(4), mid_on(1), on(3)
    last(5), mid(2), last(6), on(4)
    last(7), mid_on(2), on(5)
    last(8), mid(3), on(6), zed(1)
    project(0, (0, 1, 2, 3))
    last(9), on(7), last(10), mid_on(3), on(8)
    last(11), zed_on(1), on(9)
    last(12), mid(4), on(10)
    project(1, (0, 1, 2, 3))
    last(13), on(11), last(14), mid_on(4), on(12)
    last(15), on(13)
    last(16), mid(5), on(14)
    project(2, (0, 1, 2, 3))
    last(17), on(15), last(18), mid_on(5), last(19), last(20)
    project(3, (0, 1, 2))
    on(16)
    project(3, (3,))
    keys_values(0), keys_values(1)
    attend(0)
    last(21), on(17), mid(6)
    attend(1)
    step(0)
    on(18), last(22), mid_on(6), on(19)
    for n in range(1, 10):
        step(n)
        last(n + 22), on(n + 19)
        if n == 2:
            mid(7)
        if n == 4:
            mid_on(7)
    for i in range(29, 32):
        on(i)
    for n in range(10, 20):
        step(n)
    for s in range(2):
        for st in streams[s]:
            st.drain()
    for stage, ref in enumerate((give, pair, total.at[:, :SEQ])):
        pltpu.make_async_remote_copy(
            src_ref=ref,
            dst_ref=ref,
            send_sem=sum_sent.at[stage],
            recv_sem=sum_recv.at[stage, 0],
            device_id={"tensor": sibling},
            device_id_type=MESH,
        ).wait_send()
    pltpu.make_async_copy(out, out, io.at[1]).wait()


def tables():
    half = HEAD_DIM // 2
    frequency = np.exp(-math.log(ROPE_BASE) * np.arange(half) * 2.0 / HEAD_DIM)
    angles = np.arange(SEQ)[:, None] * frequency[None, :]
    cosine, sine = np.cos(angles), np.sin(angles)
    return (
        np.concatenate([cosine, cosine], axis=1).astype(np.float32),
        np.concatenate([-sine, sine], axis=1).astype(np.float32),
    )


def layer(activations, gain, *weights):
    vmem = pl.BlockSpec(memory_space=pltpu.VMEM)
    hbm = pl.BlockSpec(memory_space=pltpu.HBM)
    tokens, features = activations.shape
    cosine, sine = tables()
    kind = jnp.bfloat16
    chunks = features // 256
    return pl.pallas_call(
        layer_kernel,
        out_shape=jax.ShapeDtypeStruct((tokens, features), kind),
        in_specs=[hbm] + [vmem] * 11,
        out_specs=hbm,
        scratch_shapes=[
            pltpu.VMEM((tokens, features), kind),
            pltpu.VMEM((features, 640), kind),
            pltpu.VMEM((features, 640), kind),
            pltpu.VMEM((features, 512), kind),
            pltpu.VMEM((features, 512), kind),
            pltpu.VMEM((tokens, 640), jnp.float32),
            pltpu.VMEM((tokens, 640), jnp.float32),
            pltpu.VMEM((tokens, HEAD_DIM), kind),
            pltpu.VMEM((tokens, HEAD_DIM), kind),
            pltpu.VMEM((tokens, 1024), kind),
            pltpu.VMEM((chunks, SEQ, 256), kind),
            pltpu.VMEM((chunks, SEQ, 256), kind),
            pltpu.VMEM((chunks, SEQ, 256), kind),
            pltpu.VMEM((chunks, SEQ, 256), kind),
            pltpu.VMEM((chunks, SEQ, 256), kind),
            pltpu.VMEM((chunks, tokens, 256), kind),
            pltpu.VMEM((1, features), jnp.float32),
            pltpu.VMEM((1024, 64), kind),
            pltpu.SemaphoreType.DMA((2, 2, 64)),
            pltpu.SemaphoreType.DMA((2, 2)),
            pltpu.SemaphoreType.DMA((3, 16)),
            pltpu.SemaphoreType.DMA((3,)),
            pltpu.SemaphoreType.DMA((2,)),
        ],
        compiler_params=pltpu.CompilerParams(
            collective_id=0, has_side_effects=True, vmem_limit_bytes=60 * 2**20
        ),
    )(activations, gain, cosine, sine, *weights)


def shards(activations, norm_gain, *weights):
    return layer(activations, norm_gain.reshape(32, 128), *weights)


def solution(mesh):
    placed = (
        P("dp", None),
        P(),
        P("dp", None, "tensor"),
        P("dp", None, "tensor"),
        P("dp", None, "tensor"),
        P("dp", None, "tensor"),
        P("dp", None, "tensor"),
        P("dp", None, "tensor"),
        P("tensor", None, "dp"),
        P("tensor", None, "dp"),
    )
    return jax.shard_map(
        shards, mesh=mesh, in_specs=placed, out_specs=P("dp", None), check_vma=False
    )
```

```python
import math

import jax
import jax.numpy as jnp
import numpy as np
from jax import lax
from jax.experimental import pallas as pl
from jax.experimental.pallas import tpu as pltpu
from jax.sharding import PartitionSpec as P

HEAD_DIM = 128
SEQ = 256
EPS = 1e-05
ROPE_BASE = 500000.0
MESH = pl.DeviceIdType.MESH
OFF = (0, -1, 1, 2)
ROWS = 64


def turn(v, d):
    return lax.rem(v + (d + 4), 4)


class Half:
    def __init__(self, half, buf, recv, send, place, spins, toward):
        self.half, self.buf, self.recv, self.sent = half, buf, recv, send
        self.spins, self.toward = spins, toward
        x, y, z = place
        self.z = z
        self.m, self.l = (x, y) if half == 0 else (y, x)
        self.waited = {(0, 0, 0)}

    def index(self, m, l, z):
        return l * 16 + z * 4 + m if self.half == 0 else m * 16 + z * 4 + l

    def slot(self, key):
        r, jm, jl = key
        return self.index(turn(self.m, OFF[jm]), turn(self.l, OFF[jl]), turn(self.z, self.spins[r]))

    def rows(self, key):
        return self.buf.at[pl.ds(pl.multiple_of(self.slot(key) * ROWS, ROWS), ROWS)]

    def copy(self, key, device):
        return pltpu.make_async_remote_copy(
            src_ref=self.rows(key),
            dst_ref=self.rows(key),
            send_sem=self.sent,
            recv_sem=self.recv.at[self.slot(key)],
            device_id={"dp": device},
            device_id_type=MESH,
        )

    def near(self, dim, d):
        m, l, z = self.m, self.l, self.z
        if dim == "z":
            z = turn(z, d)
        elif dim == "m":
            m = turn(m, d)
        else:
            l = turn(l, d)
        return self.index(m, l, z)

    def ensure(self, key):
        if key not in self.waited:
            self.waited.add(key)
            self.copy(key, self.near("m", 1)).wait_recv()

    def both(self, key, dim):
        self.ensure(key)
        self.copy(key, self.near(dim, 1)).start()
        self.copy(key, self.near(dim, -1)).start()

    def forward(self, key_minus, key_plus, dim, way):
        if way % 2 == 0:
            self.ensure(key_minus)
            self.copy(key_minus, self.near(dim, 1)).start()
        else:
            self.ensure(key_plus)
            self.copy(key_plus, self.near(dim, -1)).start()

    def start(self):
        self.both((0, 0, 0), "z")

    def start_on(self):
        self.ensure((1, 0, 0))
        self.copy((1, 0, 0), self.near("z", self.toward)).start()

    def mid(self, r):
        self.both((r, 0, 0), "m")

    def mid_on(self, r):
        self.forward((r, 1, 0), (r, 2, 0), "m", r)

    def last(self, r, j):
        self.both((r, j, 0), "l")

    def last_on(self, r, j):
        self.forward((r, j, 1), (r, j, 2), "l", j)

    def drain(self):
        part = self.buf.at[pl.ds(0, 63 * ROWS)]
        pltpu.make_async_remote_copy(
            src_ref=part,
            dst_ref=part,
            send_sem=self.sent,
            recv_sem=self.recv.at[0],
            device_id={"dp": self.near("m", 1)},
            device_id_type=MESH,
        ).wait_send()


def product(a, b):
    return jnp.dot(a, b, preferred_element_type=jnp.float32)


def product_t(a, b):
    return lax.dot_general(a, b, (((1,), (1,)), ((), ())), preferred_element_type=jnp.float32)


def layer_kernel(
    act_in,
    gain,
    cosine,
    sine,
    query_in,
    query_exp,
    key_in,
    key_exp,
    value_in,
    value_exp,
    output_in,
    output_exp,
    out,
    raw,
    act,
    qa,
    qb,
    oa,
    ob,
    acc_a,
    acc_b,
    keys,
    values,
    context,
    give,
    keep,
    got,
    pair,
    over,
    total,
    gain_row,
    flat,
    recv,
    sent,
    sum_recv,
    sum_sent,
    swap_recv,
    swap_sent,
    io,
):
    dp = lax.axis_index("dp")
    tensor = lax.axis_index("tensor")
    x, z, y = lax.rem(dp, 4), lax.rem(dp // 4, 4), dp // 16
    core = lax.rem(tensor, 2)
    side = tensor // 2
    sibling = {"tensor": tensor + 1 - 2 * core}
    twin = {"tensor": lax.rem(tensor + 2, 4)}
    peer = {
        "dp": y * 16 + lax.rem(z + 3 - 2 * side, 4) * 4 + x,
        "tensor": lax.rem(tensor + 2, 4),
    }
    mine = pl.ds(pl.multiple_of(core * SEQ, SEQ), SEQ)
    other = pl.ds(pl.multiple_of((1 - core) * SEQ, SEQ), SEQ)

    def quarter(sequence, half):
        return pl.ds(pl.multiple_of(sequence * SEQ + half * 128, 128), 128)

    bufs = ((qa, qb), (oa, ob))
    spins = ((0, -1, 1, 2), (0, 3 + 2 * side, 1 + side, 2 + side))
    twin_spins = (0, 5 - 2 * side, 2 - side, 3 - side)
    streams = [
        [
            Half(
                h,
                bufs[k][h],
                recv.at[k, h],
                sent.at[k, h],
                (x, y, z),
                spins[k],
                (1, 1 + 2 * side)[k],
            )
            for h in range(2)
        ]
        for k in range(2)
    ]
    first = streams[0][0]
    kept = pl.ds(pl.multiple_of(side * SEQ, SEQ), SEQ)
    load_act = pltpu.make_async_copy(act_in.at[kept], raw.at[:SEQ], io.at[0])
    load_act.start()
    barrier = pltpu.get_barrier_semaphore()
    for dim in ("m", "l", "z"):
        for d in (1, -1):
            pl.semaphore_signal(
                barrier, inc=1, device_id={"dp": first.near(dim, d)}, device_id_type=MESH
            )
    for device in (sibling, twin, peer):
        pl.semaphore_signal(barrier, inc=1, device_id=device, device_id_type=MESH)

    def factor(exponents):
        return jnp.exp2(exponents.astype(jnp.float32)).astype(jnp.bfloat16)

    for b in range(2):
        rows = pl.ds(pl.multiple_of(dp * ROWS + b * 32, 32), 32)
        query = query_in[b] * factor(query_exp[b])
        qa[rows, :512] = query[:, :512]
        qb[rows, :512] = query[:, 512:]
        qa[rows, 512:] = key_in[b] * factor(key_exp[b])
        qb[rows, 512:] = value_in[b] * factor(value_exp[b])

    def fill_output():
        for b in range(32):
            flat[b * 32 : (b + 1) * 32, :] = output_in[b] * factor(output_exp[b])
        rows = pl.ds(pl.multiple_of(dp * ROWS, ROWS), ROWS)
        oa[rows, :] = flat[:512, :].T
        ob[rows, :] = flat[512:, :].T

    def fill_gain():
        for k in range(32):
            gain_row[:, k * 128 : (k + 1) * 128] = gain[k : k + 1, :].astype(jnp.float32)
        acc_a[...] = jnp.zeros_like(acc_a)
        acc_b[...] = jnp.zeros_like(acc_b)

    fill_output()
    pl.semaphore_wait(barrier, 9)

    def swap_copy(stage, p, source, half, device):
        piece = pl.ds(pl.multiple_of(source * SEQ + half * 128 + p * 32, 32), 32)
        there = pl.ds(pl.multiple_of(SEQ + half * 128 + p * 32, 32), 32)
        return pltpu.make_async_remote_copy(
            src_ref=raw.at[piece],
            dst_ref=raw.at[there],
            send_sem=swap_sent.at[stage],
            recv_sem=swap_recv.at[stage, p],
            device_id=device,
            device_id_type=MESH,
        )

    def swap(p):
        swap_copy(0, p, 0, core, peer).start()

    def swap_on(p):
        swap_copy(0, p, 0, core, peer).wait_recv()
        swap_copy(1, p, 1, core, sibling).start()

    def swap_done():
        for p in range(4):
            swap_copy(1, p, 1, 1 - core, sibling).wait_recv()

    def norm(k):
        @pl.loop(0, 8)
        def _(i):
            rows = pl.ds(pl.multiple_of(k * 128 + i * 16, 16), 16)
            wide = raw[rows, :].astype(jnp.float32)
            mean = jnp.mean(wide * wide, axis=-1, keepdims=True)
            scaled = wide * lax.rsqrt(mean + EPS) * gain_row[...]
            act[rows, :] = scaled.astype(jnp.bfloat16)

    def need(s, r, k):
        for j in range(4):
            streams[s][0].ensure((r, j, k))
        for j in range(4):
            streams[s][1].ensure((r, k, j))

    def project(r, parts):
        for k in parts:
            need(0, r, k)
        zs = turn(z, OFF[r])

        @pl.loop(parts[0], parts[-1] + 1)
        def _(k):
            away = 3 * k + 3 * (k // 2) + 2 * (k // 3)
            spot = lax.rem(y + away, 4) * 4 + zs
            part = pl.ds(pl.multiple_of(spot * 256, 256), 256)
            acc_a[...] += product(act[:, part], qa[part, :])
            acc_b[...] += product(act[:, part], qb[part, :])

    def rotate(states):
        return states * cosine[...] + pltpu.roll(states, HEAD_DIM // 2, 1) * sine[...]

    def keys_values(s):
        rows = pl.ds(s * SEQ, SEQ)
        keys[rows, :] = rotate(acc_a[rows, 512:]).astype(jnp.bfloat16)
        values[rows, :] = acc_b[rows, 512:].astype(jnp.bfloat16)

    def attend(h, s):
        acc = (acc_a, acc_b)[h]
        rows = pl.ds(s * SEQ, SEQ)
        spot = lax.broadcasted_iota(jnp.int32, (SEQ, SEQ), 0)
        seen = lax.broadcasted_iota(jnp.int32, (SEQ, SEQ), 1)
        for k in range(4):
            queries = rotate(acc[rows, k * HEAD_DIM : (k + 1) * HEAD_DIM])
            scores = product_t(queries.astype(jnp.bfloat16), keys[rows, :])
            scores = scores * HEAD_DIM ** (-0.5)
            scores = jnp.where(spot >= seen, scores, -jnp.inf)
            raised = jnp.exp(scores - jnp.max(scores, axis=-1, keepdims=True))
            weights = raised * (1.0 / jnp.sum(raised, axis=-1, keepdims=True))
            wide = product(weights.astype(jnp.bfloat16), values[rows, :]).astype(jnp.bfloat16)
            place = slice(h * 512 + k * HEAD_DIM, h * 512 + (k + 1) * HEAD_DIM)
            context[s * 128 : s * 128 + 128, place] = wide[:128]
            context[SEQ + s * 128 : SEQ + s * 128 + 128, place] = wide[128:]

    def block(n, turns=spins[1]):
        return turn(y, OFF[n % 4]) * 4 + turn(z, turns[n // 4])

    def twin_block(n):
        return block(n, twin_spins)

    def sum_copy(stage, c, src, dst, device):
        return pltpu.make_async_remote_copy(
            src_ref=src,
            dst_ref=dst,
            send_sem=sum_sent.at[stage],
            recv_sem=sum_recv.at[stage, c],
            device_id=device,
            device_id_type=MESH,
        )

    def hand(n):
        c = block(n)
        return sum_copy(0, c, give.at[c], got.at[c], sibling)

    def cross(n):
        c = block(n)
        return sum_copy(1, c, pair.at[c, 128:], over.at[c], peer)

    def spread(stage, c, sequence, half, device):
        piece = total.at[c, quarter(sequence, half)]
        return sum_copy(stage, c, piece, piece, device)

    def put(c, sequence):
        rows = pl.ds(pl.multiple_of(sequence * SEQ, SEQ), SEQ)
        columns = pl.ds(pl.multiple_of(c * 256, 256), 256)
        return pltpu.make_async_copy(total.at[c, rows], out.at[rows, columns], io.at[1])

    def partial(n, rows):
        part = pl.ds(pl.multiple_of(block(n) * 256, 256), 256)
        wide = product_t(context[rows, :512], oa[part, :]) + product_t(
            context[rows, 512:], ob[part, :]
        )
        return wide.astype(jnp.bfloat16)

    def pairs(n):
        c = block(n)
        hand(n).wait_recv()
        wide = keep[c].astype(jnp.float32) + got[c].astype(jnp.float32)
        pair[c] = wide.astype(jnp.bfloat16)

    def totals(n):
        c = block(n)
        cross(n).wait_recv()
        wide = pair[c, :128, :].astype(jnp.float32) + over[c].astype(jnp.float32)
        total[c, quarter(side, core), :] = wide.astype(jnp.bfloat16)

    def due(n):
        return tuple(m for m in range(16) if n == (m + 9 if m < 4 else m + 4))

    def tell(m):
        spread(3, block(m), side, core, twin).start()
        spread(2, block(m), side, core, sibling).start()

    def relay(m):
        spread(3, twin_block(m), 1 - side, core, twin).wait_recv()
        spread(4, twin_block(m), 1 - side, core, sibling).start()

    def finish(m):
        spread(2, block(m), side, 1 - core, sibling).wait_recv()
        put(block(m), side).start()
        spread(4, twin_block(m), 1 - side, 1 - core, sibling).wait_recv()
        put(twin_block(m), 1 - side).start()

    def step(n):
        need(1, n // 4, n % 4)
        if n >= 2:
            pairs(n - 2)
        for m in due(n):
            totals(m)
        give[block(n)] = partial(n, other)
        if n >= 2:
            cross(n - 2).start()
        for m in due(n):
            tell(m)
        for m in due(n - 4):
            relay(m)
        for m in due(n - 6):
            finish(m)
        keep[block(n)] = partial(n, mine)
        hand(n).start()

    def each(i, call):
        for st in streams[i]:
            call(st)

    def last(i):
        each(i // 16, lambda st: st.last((i // 4) % 4, i % 4))

    def on(i):
        each(i // 16, lambda st: st.last_on((i // 4) % 4, i % 4))

    def mid(q):
        each(q // 4, lambda st: st.mid(q % 4))

    def mid_on(q):
        each(q // 4, lambda st: st.mid_on(q % 4))

    def start(s):
        each(s, lambda st: st.start())

    def start_on(s):
        each(s, lambda st: st.start_on())

    whole = (0, 1, 2, 3)
    mid(0), last(0), start(0), mid(4), last(16)
    fill_gain()
    load_act.wait()
    swap(0), swap(1)
    norm(0), norm(1)
    mid_on(0), last(1), last(2), on(0)
    last(3), on(1), mid(1), start_on(0)
    swap(2), swap(3)
    on(2), last(4), mid_on(1), on(3)
    last(5), mid(2), last(6), on(4)
    swap_on(0)
    last(7), mid_on(2), on(5)
    last(8), mid(3), on(6)
    swap_on(1)
    last(9), on(7), last(10), mid_on(3), on(8)
    swap_on(2)
    last(11), on(9), start(1)
    last(12), on(10)
    swap_on(3)
    last(13), on(11), last(14)
    swap_done()
    norm(2), norm(3)
    mid_on(4), on(12)
    project(0, whole)
    last(15), on(13)
    project(1, whole)
    on(14), start_on(1)
    project(2, whole)
    last(17), on(15), last(18), last(19)
    project(3, (0, 1, 2))
    on(16), mid(5)
    project(3, (3,))
    keys_values(0), keys_values(1)
    attend(0, 0)
    on(17), last(20)
    attend(0, 1)
    on(18), mid_on(5)
    attend(1, 0)
    on(19), last(21)
    attend(1, 1)
    step(0), last(22), mid(6), on(20)
    step(1), last(23), on(21)
    step(2), last(24), mid_on(6), on(22)
    step(3), last(25), mid(7), on(23)
    step(4), last(26), on(24)
    step(5), last(27), mid_on(7), on(25)
    step(6), last(28), on(26)
    step(7), last(29), on(27)
    step(8), last(30), on(28)
    step(9), last(31), on(29)
    step(10), on(30)
    step(11), on(31)
    for n in range(12, 16):
        step(n)
    pairs(14), pairs(15)
    cross(14).start(), relay(3), cross(15).start()
    totals(12), relay(8), tell(12)
    totals(13), relay(9), tell(13)
    totals(14), relay(10), tell(14)
    totals(15), relay(11), tell(15)
    for m in (1, 2, 3, 6, 7, 8, 9, 10):
        finish(m)
    relay(12), finish(11), relay(13), finish(12), relay(14), finish(13), relay(15)
    finish(14), finish(15)
    for s in range(2):
        for st in streams[s]:
            st.drain()
    part = total.at[:, :128]
    for stage, ref in enumerate((give, pair.at[:, 128:], part, part, part)):
        sum_copy(stage, 0, ref, ref, sibling).wait_send()
    part = raw.at[:128]
    for stage in range(2):
        pltpu.make_async_remote_copy(
            src_ref=part,
            dst_ref=part,
            send_sem=swap_sent.at[stage],
            recv_sem=swap_recv.at[stage, 0],
            device_id=sibling,
            device_id_type=MESH,
        ).wait_send()
    pltpu.make_async_copy(out, out, io.at[1]).wait()


def tables():
    half = HEAD_DIM // 2
    frequency = np.exp(-math.log(ROPE_BASE) * np.arange(half) * 2.0 / HEAD_DIM)
    angles = np.arange(SEQ)[:, None] * frequency[None, :]
    cosine, sine = np.cos(angles), np.sin(angles)
    return (
        np.concatenate([cosine, cosine], axis=1).astype(np.float32),
        np.concatenate([-sine, sine], axis=1).astype(np.float32),
    )


def layer(activations, gain, *weights):
    vmem = pl.BlockSpec(memory_space=pltpu.VMEM)
    hbm = pl.BlockSpec(memory_space=pltpu.HBM)
    tokens, features = activations.shape
    cosine, sine = tables()
    kind = jnp.bfloat16
    chunks = features // 256
    return pl.pallas_call(
        layer_kernel,
        out_shape=jax.ShapeDtypeStruct((tokens, features), kind),
        in_specs=[hbm] + [vmem] * 11,
        out_specs=hbm,
        scratch_shapes=[
            pltpu.VMEM((tokens, features), kind),
            pltpu.VMEM((tokens, features), kind),
            pltpu.VMEM((features, 640), kind),
            pltpu.VMEM((features, 640), kind),
            pltpu.VMEM((features, 512), kind),
            pltpu.VMEM((features, 512), kind),
            pltpu.VMEM((tokens, 640), jnp.float32),
            pltpu.VMEM((tokens, 640), jnp.float32),
            pltpu.VMEM((tokens, HEAD_DIM), kind),
            pltpu.VMEM((tokens, HEAD_DIM), kind),
            pltpu.VMEM((tokens, 1024), kind),
            pltpu.VMEM((chunks, SEQ, 256), kind),
            pltpu.VMEM((chunks, SEQ, 256), kind),
            pltpu.VMEM((chunks, SEQ, 256), kind),
            pltpu.VMEM((chunks, SEQ, 256), kind),
            pltpu.VMEM((chunks, 128, 256), kind),
            pltpu.VMEM((chunks, tokens, 256), kind),
            pltpu.VMEM((1, features), jnp.float32),
            pltpu.VMEM((1024, 64), kind),
            pltpu.SemaphoreType.DMA((2, 2, 64)),
            pltpu.SemaphoreType.DMA((2, 2)),
            pltpu.SemaphoreType.DMA((5, 16)),
            pltpu.SemaphoreType.DMA((5,)),
            pltpu.SemaphoreType.DMA((2, 4)),
            pltpu.SemaphoreType.DMA((2,)),
            pltpu.SemaphoreType.DMA((2,)),
        ],
        compiler_params=pltpu.CompilerParams(
            collective_id=0, has_side_effects=True, vmem_limit_bytes=60 * 2**20
        ),
    )(activations, gain, cosine, sine, *weights)


def shards(activations, norm_gain, *weights):
    return layer(activations, norm_gain.reshape(32, 128), *weights)


def solution(mesh):
    placed = (
        P("dp", None),
        P(),
        P("dp", None, "tensor"),
        P("dp", None, "tensor"),
        P("dp", None, "tensor"),
        P("dp", None, "tensor"),
        P("dp", None, "tensor"),
        P("dp", None, "tensor"),
        P("tensor", None, "dp"),
        P("tensor", None, "dp"),
    )
    return jax.shard_map(
        shards, mesh=mesh, in_specs=placed, out_specs=P("dp", None), check_vma=False
    )
```

```python
import math

import jax
import jax.numpy as jnp
import numpy as np
from jax import lax
from jax.experimental import pallas as pl
from jax.experimental.pallas import tpu as pltpu
from jax.sharding import PartitionSpec as P

HEAD_DIM = 128
SEQ = 256
EPS = 1e-05
ROPE_BASE = 500000.0
MESH = pl.DeviceIdType.MESH
OFF = (0, -1, 1, 2)
ROWS = 64


def turn(v, d):
    return lax.rem(v + (d + 4), 4)


class Half:
    def __init__(self, half, buf, recv, send, place, spins, toward):
        self.half, self.buf, self.recv, self.sent = half, buf, recv, send
        self.spins, self.toward = spins, toward
        x, y, z = place
        self.z = z
        self.m, self.l = (x, y) if half == 0 else (y, x)
        self.waited = {(0, 0, 0)}

    def index(self, m, l, z):
        return l * 16 + z * 4 + m if self.half == 0 else m * 16 + z * 4 + l

    def slot(self, key):
        r, jm, jl = key
        return self.index(turn(self.m, OFF[jm]), turn(self.l, OFF[jl]), turn(self.z, self.spins[r]))

    def rows(self, key):
        return self.buf.at[pl.ds(pl.multiple_of(self.slot(key) * ROWS, ROWS), ROWS)]

    def copy(self, key, device):
        return pltpu.make_async_remote_copy(
            src_ref=self.rows(key),
            dst_ref=self.rows(key),
            send_sem=self.sent,
            recv_sem=self.recv.at[self.slot(key)],
            device_id={"dp": device},
            device_id_type=MESH,
        )

    def near(self, dim, d):
        m, l, z = self.m, self.l, self.z
        if dim == "z":
            z = turn(z, d)
        elif dim == "m":
            m = turn(m, d)
        else:
            l = turn(l, d)
        return self.index(m, l, z)

    def ensure(self, key):
        if key not in self.waited:
            self.waited.add(key)
            self.copy(key, self.near("m", 1)).wait_recv()

    def both(self, key, dim):
        self.ensure(key)
        self.copy(key, self.near(dim, 1)).start()
        self.copy(key, self.near(dim, -1)).start()

    def forward(self, key_minus, key_plus, dim, way):
        if way % 2 == 0:
            self.ensure(key_minus)
            self.copy(key_minus, self.near(dim, 1)).start()
        else:
            self.ensure(key_plus)
            self.copy(key_plus, self.near(dim, -1)).start()

    def start(self):
        self.both((0, 0, 0), "z")

    def start_on(self):
        self.ensure((1, 0, 0))
        self.copy((1, 0, 0), self.near("z", self.toward)).start()

    def mid(self, r):
        self.both((r, 0, 0), "m")

    def mid_on(self, r):
        self.forward((r, 1, 0), (r, 2, 0), "m", r)

    def last(self, r, j):
        self.both((r, j, 0), "l")

    def last_on(self, r, j):
        self.forward((r, j, 1), (r, j, 2), "l", j)

    def drain(self):
        part = self.buf.at[pl.ds(0, 63 * ROWS)]
        pltpu.make_async_remote_copy(
            src_ref=part,
            dst_ref=part,
            send_sem=self.sent,
            recv_sem=self.recv.at[0],
            device_id={"dp": self.near("m", 1)},
            device_id_type=MESH,
        ).wait_send()


def product(a, b):
    return jnp.dot(a, b, preferred_element_type=jnp.float32)


def product_t(a, b):
    return lax.dot_general(a, b, (((1,), (1,)), ((), ())), preferred_element_type=jnp.float32)


def layer_kernel(
    act_in,
    gain_hbm,
    cosine_hbm,
    sine_hbm,
    query_in_hbm,
    query_exp_hbm,
    key_in_hbm,
    key_exp_hbm,
    value_in_hbm,
    value_exp_hbm,
    output_in_hbm,
    output_exp_hbm,
    out,
    raw,
    act,
    qa,
    qb,
    oa,
    ob,
    acc_a,
    acc_b,
    keys,
    values,
    context,
    give,
    keep,
    got,
    pair,
    over,
    total,
    gain_row,
    flat,
    gain,
    cosine,
    sine,
    query_in,
    query_exp,
    key_in,
    key_exp,
    value_in,
    value_exp,
    output_in,
    output_exp,
    recv,
    sent,
    sum_recv,
    sum_sent,
    swap_recv,
    swap_sent,
    io,
):
    dp = lax.axis_index("dp")
    tensor = lax.axis_index("tensor")
    x, z, y = lax.rem(dp, 4), lax.rem(dp // 4, 4), dp // 16
    core = lax.rem(tensor, 2)
    side = tensor // 2
    sibling = {"tensor": tensor + 1 - 2 * core}
    twin = {"tensor": lax.rem(tensor + 2, 4)}
    peer = {
        "dp": y * 16 + lax.rem(z + 3 - 2 * side, 4) * 4 + x,
        "tensor": lax.rem(tensor + 2, 4),
    }
    mine = pl.ds(pl.multiple_of(core * SEQ, SEQ), SEQ)
    other = pl.ds(pl.multiple_of((1 - core) * SEQ, SEQ), SEQ)

    def quarter(sequence, half):
        return pl.ds(pl.multiple_of(sequence * SEQ + half * 128, 128), 128)

    bufs = ((qa, qb), (oa, ob))
    spins = ((0, -1, 1, 2), (0, 3 + 2 * side, 1 + side, 2 + side))
    twin_spins = (0, 5 - 2 * side, 2 - side, 3 - side)
    streams = [
        [
            Half(
                h,
                bufs[k][h],
                recv.at[k, h],
                sent.at[k, h],
                (x, y, z),
                spins[k],
                (1, 1 + 2 * side)[k],
            )
            for h in range(2)
        ]
        for k in range(2)
    ]
    first = streams[0][0]
    kept = pl.ds(pl.multiple_of(side * SEQ, SEQ), SEQ)
    load_act = pltpu.make_async_copy(act_in.at[kept], raw.at[:SEQ], io.at[0])
    loads = [
        pltpu.make_async_copy(src, dst, io.at[k + 2])
        for k, (src, dst) in enumerate(
            (
                (query_in_hbm, query_in),
                (query_exp_hbm, query_exp),
                (key_in_hbm, key_in),
                (key_exp_hbm, key_exp),
                (value_in_hbm, value_in),
                (value_exp_hbm, value_exp),
                (output_in_hbm, output_in),
                (output_exp_hbm, output_exp),
                (gain_hbm, gain),
                (cosine_hbm, cosine),
                (sine_hbm, sine),
            )
        )
    ]
    for load in loads:
        load.start()
    load_act.start()
    barrier = pltpu.get_barrier_semaphore()
    for dim in ("m", "l", "z"):
        for d in (1, -1):
            pl.semaphore_signal(
                barrier, inc=1, device_id={"dp": first.near(dim, d)}, device_id_type=MESH
            )
    for device in (sibling, twin, peer):
        pl.semaphore_signal(barrier, inc=1, device_id=device, device_id_type=MESH)

    def factor(exponents):
        return jnp.exp2(exponents.astype(jnp.float32)).astype(jnp.bfloat16)

    for load in loads:
        load.wait()
    for b in range(2):
        rows = pl.ds(pl.multiple_of(dp * ROWS + b * 32, 32), 32)
        query = query_in[b] * factor(query_exp[b])
        qa[rows, :512] = query[:, :512]
        qb[rows, :512] = query[:, 512:]
        qa[rows, 512:] = key_in[b] * factor(key_exp[b])
        qb[rows, 512:] = value_in[b] * factor(value_exp[b])

    def fill_output():
        for b in range(32):
            flat[b * 32 : (b + 1) * 32, :] = output_in[b] * factor(output_exp[b])
        rows = pl.ds(pl.multiple_of(dp * ROWS, ROWS), ROWS)
        oa[rows, :] = flat[:512, :].T
        ob[rows, :] = flat[512:, :].T

    def fill_gain():
        for k in range(32):
            gain_row[:, k * 128 : (k + 1) * 128] = gain[k : k + 1, :].astype(jnp.float32)
        acc_a[...] = jnp.zeros_like(acc_a)
        acc_b[...] = jnp.zeros_like(acc_b)

    fill_output()
    pl.semaphore_wait(barrier, 9)

    def swap_copy(stage, p, source, half, device):
        piece = pl.ds(pl.multiple_of(source * SEQ + half * 128 + p * 32, 32), 32)
        there = pl.ds(pl.multiple_of(SEQ + half * 128 + p * 32, 32), 32)
        return pltpu.make_async_remote_copy(
            src_ref=raw.at[piece],
            dst_ref=raw.at[there],
            send_sem=swap_sent.at[stage],
            recv_sem=swap_recv.at[stage, p],
            device_id=device,
            device_id_type=MESH,
        )

    def swap(p):
        swap_copy(0, p, 0, core, peer).start()

    def swap_on(p):
        swap_copy(0, p, 0, core, peer).wait_recv()
        swap_copy(1, p, 1, core, sibling).start()

    def swap_done():
        for p in range(4):
            swap_copy(1, p, 1, 1 - core, sibling).wait_recv()

    def norm(k):
        @pl.loop(0, 8)
        def _(i):
            rows = pl.ds(pl.multiple_of(k * 128 + i * 16, 16), 16)
            wide = raw[rows, :].astype(jnp.float32)
            mean = jnp.mean(wide * wide, axis=-1, keepdims=True)
            scaled = wide * lax.rsqrt(mean + EPS) * gain_row[...]
            act[rows, :] = scaled.astype(jnp.bfloat16)

    def need(s, r, k):
        for j in range(4):
            streams[s][0].ensure((r, j, k))
        for j in range(4):
            streams[s][1].ensure((r, k, j))

    def project(r, parts):
        for k in parts:
            need(0, r, k)
        zs = turn(z, OFF[r])

        @pl.loop(parts[0], parts[-1] + 1)
        def _(k):
            away = 3 * k + 3 * (k // 2) + 2 * (k // 3)
            spot = lax.rem(y + away, 4) * 4 + zs
            part = pl.ds(pl.multiple_of(spot * 256, 256), 256)
            acc_a[...] += product(act[:, part], qa[part, :])
            acc_b[...] += product(act[:, part], qb[part, :])

    def rotate(states):
        return states * cosine[...] + pltpu.roll(states, HEAD_DIM // 2, 1) * sine[...]

    def keys_values(s):
        rows = pl.ds(s * SEQ, SEQ)
        keys[rows, :] = rotate(acc_a[rows, 512:]).astype(jnp.bfloat16)
        values[rows, :] = acc_b[rows, 512:].astype(jnp.bfloat16)

    def attend(h, s):
        acc = (acc_a, acc_b)[h]
        rows = pl.ds(s * SEQ, SEQ)
        spot = lax.broadcasted_iota(jnp.int32, (SEQ, SEQ), 0)
        seen = lax.broadcasted_iota(jnp.int32, (SEQ, SEQ), 1)
        for k in range(4):
            queries = rotate(acc[rows, k * HEAD_DIM : (k + 1) * HEAD_DIM])
            scores = product_t(queries.astype(jnp.bfloat16), keys[rows, :])
            scores = scores * HEAD_DIM ** (-0.5)
            scores = jnp.where(spot >= seen, scores, -jnp.inf)
            raised = jnp.exp(scores - jnp.max(scores, axis=-1, keepdims=True))
            weights = raised * (1.0 / jnp.sum(raised, axis=-1, keepdims=True))
            wide = product(weights.astype(jnp.bfloat16), values[rows, :]).astype(jnp.bfloat16)
            place = slice(h * 512 + k * HEAD_DIM, h * 512 + (k + 1) * HEAD_DIM)
            context[s * 128 : s * 128 + 128, place] = wide[:128]
            context[SEQ + s * 128 : SEQ + s * 128 + 128, place] = wide[128:]

    def block(n, turns=spins[1]):
        return turn(y, OFF[n % 4]) * 4 + turn(z, turns[n // 4])

    def twin_block(n):
        return block(n, twin_spins)

    def sum_copy(stage, c, src, dst, device):
        return pltpu.make_async_remote_copy(
            src_ref=src,
            dst_ref=dst,
            send_sem=sum_sent.at[stage],
            recv_sem=sum_recv.at[stage, c],
            device_id=device,
            device_id_type=MESH,
        )

    def hand(n):
        c = block(n)
        return sum_copy(0, c, give.at[c], got.at[c], sibling)

    def cross(n):
        c = block(n)
        return sum_copy(1, c, pair.at[c, 128:], over.at[c], peer)

    def spread(stage, c, sequence, half, device):
        piece = total.at[c, quarter(sequence, half)]
        return sum_copy(stage, c, piece, piece, device)

    def put(c, sequence):
        rows = pl.ds(pl.multiple_of(sequence * SEQ, SEQ), SEQ)
        columns = pl.ds(pl.multiple_of(c * 256, 256), 256)
        return pltpu.make_async_copy(total.at[c, rows], out.at[rows, columns], io.at[1])

    def partial(n, rows):
        part = pl.ds(pl.multiple_of(block(n) * 256, 256), 256)
        wide = product_t(context[rows, :512], oa[part, :]) + product_t(
            context[rows, 512:], ob[part, :]
        )
        return wide.astype(jnp.bfloat16)

    def pairs(n):
        c = block(n)
        hand(n).wait_recv()
        wide = keep[c].astype(jnp.float32) + got[c].astype(jnp.float32)
        pair[c] = wide.astype(jnp.bfloat16)

    def totals(n):
        c = block(n)
        cross(n).wait_recv()
        wide = pair[c, :128, :].astype(jnp.float32) + over[c].astype(jnp.float32)
        total[c, quarter(side, core), :] = wide.astype(jnp.bfloat16)

    def due(n):
        return tuple(m for m in range(16) if n == m + (8, 3, 5, 5)[m // 4])

    def tell(m):
        spread(3, block(m), side, core, twin).start()
        spread(2, block(m), side, core, sibling).start()

    def relay(m):
        spread(3, twin_block(m), 1 - side, core, twin).wait_recv()
        spread(4, twin_block(m), 1 - side, core, sibling).start()

    def finish(m):
        spread(2, block(m), side, 1 - core, sibling).wait_recv()
        put(block(m), side).start()
        spread(4, twin_block(m), 1 - side, 1 - core, sibling).wait_recv()
        put(twin_block(m), 1 - side).start()

    def step(n):
        need(1, n // 4, n % 4)
        if n >= 2:
            pairs(n - 2)
        give[block(n)] = partial(n, other)
        keep[block(n)] = partial(n, mine)
        if n >= 2:
            cross(n - 2).start()
        hand(n).start()
        for m in due(n):
            totals(m)
        for m in due(n - 4):
            relay(m)
        for m in due(n - 6):
            finish(m)
        for m in due(n):
            tell(m)

    def each(i, call):
        for st in streams[i]:
            call(st)

    def last(i):
        each(i // 16, lambda st: st.last((i // 4) % 4, i % 4))

    def on(i):
        each(i // 16, lambda st: st.last_on((i // 4) % 4, i % 4))

    def mid(q):
        each(q // 4, lambda st: st.mid(q % 4))

    def mid_on(q):
        each(q // 4, lambda st: st.mid_on(q % 4))

    def start(s):
        each(s, lambda st: st.start())

    def start_on(s):
        each(s, lambda st: st.start_on())

    whole = (0, 1, 2, 3)
    mid(0), last(0), start(0), mid(4), last(16)
    fill_gain()
    load_act.wait()
    swap(0), swap(1)
    norm(0), norm(1)
    mid_on(0), last(1), last(2), on(0)
    last(3), on(1), mid(1), start_on(0)
    swap(2), swap(3)
    on(2), last(4), mid_on(1), on(3)
    last(5), mid(2), last(6), on(4)
    swap_on(0)
    last(7), mid_on(2), on(5)
    last(8), mid(3), on(6)
    swap_on(1)
    last(9), on(7), last(10), mid_on(3), on(8)
    swap_on(2)
    last(11), on(9), start(1)
    last(12), on(10)
    swap_on(3)
    last(13), on(11), last(14)
    swap_done()
    norm(2), norm(3)
    mid_on(4), on(12)
    project(0, whole)
    last(15), on(13)
    project(1, whole)
    on(14), start_on(1)
    project(2, whole)
    last(17), on(15), last(18), last(19)
    project(3, (0, 1, 2))
    on(16), mid(5)
    project(3, (3,))
    keys_values(0), keys_values(1)
    attend(0, 0)
    on(17), last(20)
    attend(0, 1)
    on(18), mid_on(5)
    attend(1, 0)
    on(19), last(21)
    attend(1, 1)
    step(0), last(22), mid(6), on(20)
    step(1), last(23), on(21)
    step(2), last(24), mid_on(6), on(22)
    step(3), last(25), mid(7), on(23)
    step(4), last(26), on(24)
    step(5), last(27), mid_on(7), on(25)
    step(6), last(28), on(26)
    step(7), last(29), on(27)
    step(8), last(30), on(28)
    step(9), last(31), on(29)
    step(10), on(30)
    step(11), on(31)
    for n in range(12, 16):
        step(n)
    pairs(14), finish(2), finish(3), finish(7)
    cross(14).start()
    pairs(15), totals(11)
    cross(15).start(), relay(8), tell(11)
    totals(12), relay(9), tell(12)
    totals(13), finish(8), tell(13)
    totals(14), finish(9), tell(14)
    totals(15), relay(10), tell(15)
    relay(11), finish(10), relay(12), finish(11), relay(13), finish(12), relay(14)
    finish(13), relay(15), finish(14), finish(15)
    for s in range(2):
        for st in streams[s]:
            st.drain()
    part = total.at[:, :128]
    for stage, ref in enumerate((give, pair.at[:, 128:], part, part, part)):
        sum_copy(stage, 0, ref, ref, sibling).wait_send()
    part = raw.at[:128]
    for stage in range(2):
        pltpu.make_async_remote_copy(
            src_ref=part,
            dst_ref=part,
            send_sem=swap_sent.at[stage],
            recv_sem=swap_recv.at[stage, 0],
            device_id=sibling,
            device_id_type=MESH,
        ).wait_send()
    pltpu.make_async_copy(out, out, io.at[1]).wait()


def tables():
    half = HEAD_DIM // 2
    frequency = np.exp(-math.log(ROPE_BASE) * np.arange(half) * 2.0 / HEAD_DIM)
    angles = np.arange(SEQ)[:, None] * frequency[None, :]
    cosine, sine = np.cos(angles), np.sin(angles)
    return (
        np.concatenate([cosine, cosine], axis=1).astype(np.float32),
        np.concatenate([-sine, sine], axis=1).astype(np.float32),
    )


def layer(activations, gain, *weights):
    vmem = pl.BlockSpec(memory_space=pltpu.VMEM)
    hbm = pl.BlockSpec(memory_space=pltpu.HBM)
    tokens, features = activations.shape
    cosine, sine = tables()
    kind = jnp.bfloat16
    chunks = features // 256
    small = (gain, cosine, sine, *weights)
    return pl.pallas_call(
        layer_kernel,
        out_shape=jax.ShapeDtypeStruct((tokens, features), kind),
        in_specs=[hbm] * 12,
        out_specs=hbm,
        scratch_shapes=[
            pltpu.VMEM((tokens, features), kind),
            pltpu.VMEM((tokens, features), kind),
            pltpu.VMEM((features, 640), kind),
            pltpu.VMEM((features, 640), kind),
            pltpu.VMEM((features, 512), kind),
            pltpu.VMEM((features, 512), kind),
            pltpu.VMEM((tokens, 640), jnp.float32),
            pltpu.VMEM((tokens, 640), jnp.float32),
            pltpu.VMEM((tokens, HEAD_DIM), kind),
            pltpu.VMEM((tokens, HEAD_DIM), kind),
            pltpu.VMEM((tokens, 1024), kind),
            pltpu.VMEM((chunks, SEQ, 256), kind),
            pltpu.VMEM((chunks, SEQ, 256), kind),
            pltpu.VMEM((chunks, SEQ, 256), kind),
            pltpu.VMEM((chunks, SEQ, 256), kind),
            pltpu.VMEM((chunks, 128, 256), kind),
            pltpu.VMEM((chunks, tokens, 256), kind),
            pltpu.VMEM((1, features), jnp.float32),
            pltpu.VMEM((1024, 64), kind),
            *(pltpu.VMEM(a.shape, a.dtype) for a in small),
            pltpu.SemaphoreType.DMA((2, 2, 64)),
            pltpu.SemaphoreType.DMA((2, 2)),
            pltpu.SemaphoreType.DMA((5, 16)),
            pltpu.SemaphoreType.DMA((5,)),
            pltpu.SemaphoreType.DMA((2, 4)),
            pltpu.SemaphoreType.DMA((2,)),
            pltpu.SemaphoreType.DMA((13,)),
        ],
        compiler_params=pltpu.CompilerParams(
            collective_id=0, has_side_effects=True, vmem_limit_bytes=60 * 2**20
        ),
    )(activations, *small)


def shards(activations, norm_gain, *weights):
    return layer(activations, norm_gain.reshape(32, 128), *weights)


def solution(mesh):
    placed = (
        P("dp", None),
        P(),
        P("dp", None, "tensor"),
        P("dp", None, "tensor"),
        P("dp", None, "tensor"),
        P("dp", None, "tensor"),
        P("dp", None, "tensor"),
        P("dp", None, "tensor"),
        P("tensor", None, "dp"),
        P("tensor", None, "dp"),
    )
    return jax.shard_map(
        shards, mesh=mesh, in_specs=placed, out_specs=P("dp", None), check_vma=False
    )
```

```python
import math

import jax
import jax.numpy as jnp
import numpy as np
from jax import lax
from jax.experimental import pallas as pl
from jax.experimental.pallas import tpu as pltpu
from jax.sharding import PartitionSpec as P

HEAD_DIM = 128
SEQ = 256
EPS = 1e-05
ROPE_BASE = 500000.0
MESH = pl.DeviceIdType.MESH
OFF = (0, -1, 1, 2)
ROWS = 64


def turn(v, d):
    return lax.rem(v + (d + 4), 4)


class Half:
    def __init__(self, half, buf, recv, send, place, spins, toward):
        self.half, self.buf, self.recv, self.sent = half, buf, recv, send
        self.spins, self.toward = spins, toward
        x, y, z = place
        self.z = z
        self.m, self.l = (x, y) if half == 0 else (y, x)
        self.waited = {(0, 0, 0)}

    def index(self, m, l, z):
        return l * 16 + z * 4 + m if self.half == 0 else m * 16 + z * 4 + l

    def slot(self, key):
        r, jm, jl = key
        return self.index(turn(self.m, OFF[jm]), turn(self.l, OFF[jl]), turn(self.z, self.spins[r]))

    def rows(self, key):
        return self.buf.at[pl.ds(pl.multiple_of(self.slot(key) * ROWS, ROWS), ROWS)]

    def copy(self, key, device):
        return pltpu.make_async_remote_copy(
            src_ref=self.rows(key),
            dst_ref=self.rows(key),
            send_sem=self.sent,
            recv_sem=self.recv.at[self.slot(key)],
            device_id={"dp": device},
            device_id_type=MESH,
        )

    def near(self, dim, d):
        m, l, z = self.m, self.l, self.z
        if dim == "z":
            z = turn(z, d)
        elif dim == "m":
            m = turn(m, d)
        else:
            l = turn(l, d)
        return self.index(m, l, z)

    def ensure(self, key):
        if key not in self.waited:
            self.waited.add(key)
            self.copy(key, self.near("m", 1)).wait_recv()

    def both(self, key, dim):
        self.ensure(key)
        self.copy(key, self.near(dim, 1)).start()
        self.copy(key, self.near(dim, -1)).start()

    def forward(self, key_minus, key_plus, dim, way):
        if way % 2 == 0:
            self.ensure(key_minus)
            self.copy(key_minus, self.near(dim, 1)).start()
        else:
            self.ensure(key_plus)
            self.copy(key_plus, self.near(dim, -1)).start()

    def start(self):
        self.both((0, 0, 0), "z")

    def start_on(self):
        self.ensure((1, 0, 0))
        self.copy((1, 0, 0), self.near("z", self.toward)).start()

    def mid(self, r):
        self.both((r, 0, 0), "m")

    def mid_on(self, r):
        self.forward((r, 1, 0), (r, 2, 0), "m", r)

    def last(self, r, j):
        self.both((r, j, 0), "l")

    def last_on(self, r, j):
        self.forward((r, j, 1), (r, j, 2), "l", j)

    def drain(self):
        part = self.buf.at[pl.ds(0, 63 * ROWS)]
        pltpu.make_async_remote_copy(
            src_ref=part,
            dst_ref=part,
            send_sem=self.sent,
            recv_sem=self.recv.at[0],
            device_id={"dp": self.near("m", 1)},
            device_id_type=MESH,
        ).wait_send()


def product(a, b):
    return jnp.dot(a, b, preferred_element_type=jnp.float32)


def product_t(a, b):
    return lax.dot_general(a, b, (((1,), (1,)), ((), ())), preferred_element_type=jnp.float32)


def layer_kernel(
    act_in,
    gain_hbm,
    cosine_hbm,
    sine_hbm,
    query_in_hbm,
    query_exp_hbm,
    key_in_hbm,
    key_exp_hbm,
    value_in_hbm,
    value_exp_hbm,
    output_in_hbm,
    output_exp_hbm,
    total,
    raw,
    act,
    qa,
    qb,
    oa,
    ob,
    acc_a,
    acc_b,
    keys,
    values,
    context,
    give,
    keep,
    got,
    pair,
    over,
    gain_row,
    flat,
    gain,
    cosine,
    sine,
    query_in,
    query_exp,
    key_in,
    key_exp,
    value_in,
    value_exp,
    output_in,
    output_exp,
    recv,
    sent,
    sum_recv,
    sum_sent,
    swap_recv,
    swap_sent,
    io,
):
    dp = lax.axis_index("dp")
    tensor = lax.axis_index("tensor")
    x, z, y = lax.rem(dp, 4), lax.rem(dp // 4, 4), dp // 16
    core = lax.rem(tensor, 2)
    side = tensor // 2
    sibling = {"tensor": tensor + 1 - 2 * core}
    twin = {"tensor": lax.rem(tensor + 2, 4)}
    peer = {
        "dp": y * 16 + lax.rem(z + 3 - 2 * side, 4) * 4 + x,
        "tensor": lax.rem(tensor + 2, 4),
    }
    mine = pl.ds(pl.multiple_of(core * SEQ, SEQ), SEQ)
    other = pl.ds(pl.multiple_of((1 - core) * SEQ, SEQ), SEQ)

    def quarter(sequence, half):
        return pl.ds(pl.multiple_of(sequence * SEQ + half * 128, 128), 128)

    bufs = ((qa, qb), (oa, ob))
    spins = ((0, -1, 1, 2), (0, 3 + 2 * side, 1 + side, 2 + side))
    twin_spins = (0, 5 - 2 * side, 2 - side, 3 - side)
    streams = [
        [
            Half(
                h,
                bufs[k][h],
                recv.at[k, h],
                sent.at[k, h],
                (x, y, z),
                spins[k],
                (1, 1 + 2 * side)[k],
            )
            for h in range(2)
        ]
        for k in range(2)
    ]
    first = streams[0][0]
    kept = pl.ds(pl.multiple_of(side * SEQ, SEQ), SEQ)
    load_act = pltpu.make_async_copy(act_in.at[kept], raw.at[:SEQ], io.at[0])
    loads = [
        pltpu.make_async_copy(src, dst, io.at[k + 2])
        for k, (src, dst) in enumerate(
            (
                (query_in_hbm, query_in),
                (query_exp_hbm, query_exp),
                (key_in_hbm, key_in),
                (key_exp_hbm, key_exp),
                (value_in_hbm, value_in),
                (value_exp_hbm, value_exp),
                (output_in_hbm, output_in),
                (output_exp_hbm, output_exp),
                (gain_hbm, gain),
                (cosine_hbm, cosine),
                (sine_hbm, sine),
            )
        )
    ]
    for load in loads:
        load.start()
    load_act.start()
    barrier = pltpu.get_barrier_semaphore()
    for dim in ("m", "l", "z"):
        for d in (1, -1):
            pl.semaphore_signal(
                barrier, inc=1, device_id={"dp": first.near(dim, d)}, device_id_type=MESH
            )
    for device in (sibling, twin, peer):
        pl.semaphore_signal(barrier, inc=1, device_id=device, device_id_type=MESH)

    def factor(exponents):
        return jnp.exp2(exponents.astype(jnp.float32)).astype(jnp.bfloat16)

    for load in loads:
        load.wait()
    for b in range(2):
        rows = pl.ds(pl.multiple_of(dp * ROWS + b * 32, 32), 32)
        query = query_in[b] * factor(query_exp[b])
        qa[rows, :512] = query[:, :512]
        qb[rows, :512] = query[:, 512:]
        qa[rows, 512:] = key_in[b] * factor(key_exp[b])
        qb[rows, 512:] = value_in[b] * factor(value_exp[b])

    def fill_output():
        for b in range(32):
            flat[b * 32 : (b + 1) * 32, :] = output_in[b] * factor(output_exp[b])
        rows = pl.ds(pl.multiple_of(dp * ROWS, ROWS), ROWS)
        oa[rows, :] = flat[:512, :].T
        ob[rows, :] = flat[512:, :].T

    def fill_gain():
        for k in range(32):
            gain_row[:, k * 128 : (k + 1) * 128] = gain[k : k + 1, :].astype(jnp.float32)
        acc_a[...] = jnp.zeros_like(acc_a)
        acc_b[...] = jnp.zeros_like(acc_b)

    fill_output()
    pl.semaphore_wait(barrier, 9)

    def swap_copy(stage, p, source, half, device):
        piece = pl.ds(pl.multiple_of(source * SEQ + half * 128 + p * 32, 32), 32)
        there = pl.ds(pl.multiple_of(SEQ + half * 128 + p * 32, 32), 32)
        return pltpu.make_async_remote_copy(
            src_ref=raw.at[piece],
            dst_ref=raw.at[there],
            send_sem=swap_sent.at[stage],
            recv_sem=swap_recv.at[stage, p],
            device_id=device,
            device_id_type=MESH,
        )

    def swap(p):
        swap_copy(0, p, 0, core, peer).start()

    def swap_on(p):
        swap_copy(0, p, 0, core, peer).wait_recv()
        swap_copy(1, p, 1, core, sibling).start()

    def swap_done():
        for p in range(4):
            swap_copy(1, p, 1, 1 - core, sibling).wait_recv()

    def norm(k):
        @pl.loop(0, 8)
        def _(i):
            rows = pl.ds(pl.multiple_of(k * 128 + i * 16, 16), 16)
            wide = raw[rows, :].astype(jnp.float32)
            mean = jnp.mean(wide * wide, axis=-1, keepdims=True)
            scaled = wide * lax.rsqrt(mean + EPS) * gain_row[...]
            act[rows, :] = scaled.astype(jnp.bfloat16)

    def need(s, r, k):
        for j in range(4):
            streams[s][0].ensure((r, j, k))
        for j in range(4):
            streams[s][1].ensure((r, k, j))

    def project(r, parts):
        for k in parts:
            need(0, r, k)
        zs = turn(z, OFF[r])

        @pl.loop(parts[0], parts[-1] + 1)
        def _(k):
            away = 3 * k + 3 * (k // 2) + 2 * (k // 3)
            spot = lax.rem(y + away, 4) * 4 + zs
            part = pl.ds(pl.multiple_of(spot * 256, 256), 256)
            acc_a[...] += product(act[:, part], qa[part, :])
            acc_b[...] += product(act[:, part], qb[part, :])

    def rotate(states):
        return states * cosine[...] + pltpu.roll(states, HEAD_DIM // 2, 1) * sine[...]

    def keys_values(s):
        rows = pl.ds(s * SEQ, SEQ)
        keys[rows, :] = rotate(acc_a[rows, 512:]).astype(jnp.bfloat16)
        values[rows, :] = acc_b[rows, 512:].astype(jnp.bfloat16)

    def attend(h, s):
        acc = (acc_a, acc_b)[h]
        rows = pl.ds(s * SEQ, SEQ)
        spot = lax.broadcasted_iota(jnp.int32, (SEQ, SEQ), 0)
        seen = lax.broadcasted_iota(jnp.int32, (SEQ, SEQ), 1)
        for k in range(4):
            queries = rotate(acc[rows, k * HEAD_DIM : (k + 1) * HEAD_DIM])
            scores = product_t(queries.astype(jnp.bfloat16), keys[rows, :])
            scores = scores * HEAD_DIM ** (-0.5)
            scores = jnp.where(spot >= seen, scores, -jnp.inf)
            raised = jnp.exp(scores - jnp.max(scores, axis=-1, keepdims=True))
            weights = raised * (1.0 / jnp.sum(raised, axis=-1, keepdims=True))
            wide = product(weights.astype(jnp.bfloat16), values[rows, :]).astype(jnp.bfloat16)
            place = slice(h * 512 + k * HEAD_DIM, h * 512 + (k + 1) * HEAD_DIM)
            context[s * 128 : s * 128 + 128, place] = wide[:128]
            context[SEQ + s * 128 : SEQ + s * 128 + 128, place] = wide[128:]

    def block(n, turns=spins[1]):
        return turn(y, OFF[n % 4]) * 4 + turn(z, turns[n // 4])

    def twin_block(n):
        return block(n, twin_spins)

    def sum_copy(stage, c, src, dst, device):
        return pltpu.make_async_remote_copy(
            src_ref=src,
            dst_ref=dst,
            send_sem=sum_sent.at[stage],
            recv_sem=sum_recv.at[stage, c],
            device_id=device,
            device_id_type=MESH,
        )

    def hand(n):
        c = block(n)
        return sum_copy(0, c, give.at[c], got.at[c], sibling)

    def cross(n):
        c = block(n)
        return sum_copy(1, c, pair.at[c, 128:], over.at[c], peer)

    def spread(stage, c, sequence, half, device):
        piece = total.at[c, quarter(sequence, half)]
        return sum_copy(stage, c, piece, piece, device)

    def partial(n, rows):
        part = pl.ds(pl.multiple_of(block(n) * 256, 256), 256)
        wide = product_t(context[rows, :512], oa[part, :]) + product_t(
            context[rows, 512:], ob[part, :]
        )
        return wide.astype(jnp.bfloat16)

    def pairs(n):
        c = block(n)
        hand(n).wait_recv()
        wide = keep[c].astype(jnp.float32) + got[c].astype(jnp.float32)
        pair[c] = wide.astype(jnp.bfloat16)

    def totals(n):
        c = block(n)
        cross(n).wait_recv()
        wide = pair[c, :128, :].astype(jnp.float32) + over[c].astype(jnp.float32)
        total[c, quarter(side, core), :] = wide.astype(jnp.bfloat16)

    def due(n):
        return tuple(m for m in range(16) if n == m + (8, 3, 5, 5)[m // 4])

    def tell(m):
        spread(3, block(m), side, core, twin).start()
        spread(2, block(m), side, core, sibling).start()

    def relay(m):
        spread(3, twin_block(m), 1 - side, core, twin).wait_recv()
        spread(4, twin_block(m), 1 - side, core, sibling).start()

    def finish(m):
        spread(2, block(m), side, 1 - core, sibling).wait_recv()
        spread(4, twin_block(m), 1 - side, 1 - core, sibling).wait_recv()

    def step(n):
        need(1, n // 4, n % 4)
        if n >= 2:
            pairs(n - 2)
        give[block(n)] = partial(n, other)
        keep[block(n)] = partial(n, mine)
        if n >= 2:
            cross(n - 2).start()
        hand(n).start()
        for m in due(n):
            totals(m)
        for m in due(n - 4):
            relay(m)
        for m in due(n - 6):
            finish(m)
        for m in due(n):
            tell(m)

    def each(i, call):
        for st in streams[i]:
            call(st)

    def last(i):
        each(i // 16, lambda st: st.last((i // 4) % 4, i % 4))

    def on(i):
        each(i // 16, lambda st: st.last_on((i // 4) % 4, i % 4))

    def mid(q):
        each(q // 4, lambda st: st.mid(q % 4))

    def mid_on(q):
        each(q // 4, lambda st: st.mid_on(q % 4))

    def start(s):
        each(s, lambda st: st.start())

    def start_on(s):
        each(s, lambda st: st.start_on())

    whole = (0, 1, 2, 3)
    mid(0), last(0), start(0), mid(4), last(16)
    fill_gain()
    load_act.wait()
    swap(0), swap(1)
    norm(0), norm(1)
    mid_on(0), last(1), last(2), on(0)
    last(3), on(1), mid(1), start_on(0)
    swap(2), swap(3)
    on(2), last(4), mid_on(1), on(3)
    last(5), mid(2), last(6), on(4)
    swap_on(0)
    last(7), mid_on(2), on(5)
    last(8), mid(3), on(6)
    swap_on(1)
    last(9), on(7), last(10), mid_on(3), on(8)
    swap_on(2)
    last(11), on(9), start(1)
    last(12), on(10)
    swap_on(3)
    last(13), on(11), last(14)
    swap_done()
    norm(2), norm(3)
    mid_on(4), on(12)
    project(0, whole)
    last(15), on(13)
    project(1, whole)
    on(14), start_on(1)
    project(2, whole)
    last(17), on(15), last(18), last(19)
    project(3, (0, 1, 2))
    on(16), mid(5)
    project(3, (3,))
    keys_values(0), keys_values(1)
    attend(0, 0)
    on(17), last(20)
    attend(0, 1)
    on(18), mid_on(5)
    attend(1, 0)
    on(19), last(21)
    attend(1, 1)
    step(0), last(22), mid(6), on(20)
    step(1), last(23), on(21)
    step(2), last(24), mid_on(6), on(22)
    step(3), last(25), mid(7), on(23)
    step(4), last(26), on(24)
    step(5), last(27), mid_on(7), on(25)
    step(6), last(28), on(26)
    step(7), last(29), on(27)
    step(8), last(30), on(28)
    step(9), last(31), on(29)
    step(10), on(30)
    step(11), on(31)
    for n in range(12, 16):
        step(n)
    pairs(14), pairs(15)
    cross(14).start(), totals(11)
    cross(15).start(), finish(2), tell(11)
    totals(12), relay(8), tell(12)
    totals(13), relay(9), tell(13)
    totals(14), finish(3), tell(14)
    totals(15), finish(7), tell(15)
    relay(10), finish(8), finish(9)
    relay(11), finish(10), relay(12), finish(11), relay(13), finish(12), relay(14)
    finish(13), relay(15), finish(14), finish(15)
    for s in range(2):
        for st in streams[s]:
            st.drain()
    part = total.at[:, :128]
    for stage, ref in enumerate((give, pair.at[:, 128:], part, part, part)):
        sum_copy(stage, 0, ref, ref, sibling).wait_send()
    part = raw.at[:128]
    for stage in range(2):
        pltpu.make_async_remote_copy(
            src_ref=part,
            dst_ref=part,
            send_sem=swap_sent.at[stage],
            recv_sem=swap_recv.at[stage, 0],
            device_id=sibling,
            device_id_type=MESH,
        ).wait_send()


def tables():
    half = HEAD_DIM // 2
    frequency = np.exp(-math.log(ROPE_BASE) * np.arange(half) * 2.0 / HEAD_DIM)
    angles = np.arange(SEQ)[:, None] * frequency[None, :]
    cosine, sine = np.cos(angles), np.sin(angles)
    return (
        np.concatenate([cosine, cosine], axis=1).astype(np.float32),
        np.concatenate([-sine, sine], axis=1).astype(np.float32),
    )


def layer(activations, gain, *weights):
    vmem = pl.BlockSpec(memory_space=pltpu.VMEM)
    hbm = pl.BlockSpec(memory_space=pltpu.HBM)
    tokens, features = activations.shape
    cosine, sine = tables()
    kind = jnp.bfloat16
    chunks = features // 256
    small = [
        pltpu.with_memory_space_constraint(jnp.asarray(a), pltpu.HBM)
        for a in (gain, cosine, sine, *weights)
    ]
    return pl.pallas_call(
        layer_kernel,
        out_shape=jax.ShapeDtypeStruct((chunks, tokens, 256), kind),
        in_specs=[hbm] * 12,
        out_specs=vmem,
        scratch_shapes=[
            pltpu.VMEM((tokens, features), kind),
            pltpu.VMEM((tokens, features), kind),
            pltpu.VMEM((features, 640), kind),
            pltpu.VMEM((features, 640), kind),
            pltpu.VMEM((features, 512), kind),
            pltpu.VMEM((features, 512), kind),
            pltpu.VMEM((tokens, 640), jnp.float32),
            pltpu.VMEM((tokens, 640), jnp.float32),
            pltpu.VMEM((tokens, HEAD_DIM), kind),
            pltpu.VMEM((tokens, HEAD_DIM), kind),
            pltpu.VMEM((tokens, 1024), kind),
            pltpu.VMEM((chunks, SEQ, 256), kind),
            pltpu.VMEM((chunks, SEQ, 256), kind),
            pltpu.VMEM((chunks, SEQ, 256), kind),
            pltpu.VMEM((chunks, SEQ, 256), kind),
            pltpu.VMEM((chunks, 128, 256), kind),
            pltpu.VMEM((1, features), jnp.float32),
            pltpu.VMEM((1024, 64), kind),
            *(pltpu.VMEM(a.shape, a.dtype) for a in small),
            pltpu.SemaphoreType.DMA((2, 2, 64)),
            pltpu.SemaphoreType.DMA((2, 2)),
            pltpu.SemaphoreType.DMA((5, 16)),
            pltpu.SemaphoreType.DMA((5,)),
            pltpu.SemaphoreType.DMA((2, 4)),
            pltpu.SemaphoreType.DMA((2,)),
            pltpu.SemaphoreType.DMA((13,)),
        ],
        compiler_params=pltpu.CompilerParams(
            collective_id=0, has_side_effects=True, vmem_limit_bytes=48 * 2**20
        ),
    )(activations, *small)


def place_kernel(blocks, out, sent):
    copies = [
        pltpu.make_async_copy(blocks.at[c], out.at[:, pl.ds(c * 256, 256)], sent.at[c])
        for c in range(blocks.shape[0])
    ]
    for copy in copies:
        copy.start()
    for copy in copies:
        copy.wait()


def shards(activations, norm_gain, *weights):
    blocks = layer(activations, norm_gain.reshape(32, 128), *weights)
    return pl.pallas_call(
        place_kernel,
        out_shape=jax.ShapeDtypeStruct(activations.shape, activations.dtype),
        in_specs=[pl.BlockSpec(memory_space=pltpu.VMEM)],
        out_specs=pl.BlockSpec(memory_space=pltpu.HBM),
        scratch_shapes=[pltpu.SemaphoreType.DMA((blocks.shape[0],))],
        compiler_params=pltpu.CompilerParams(vmem_limit_bytes=2**20),
    )(blocks)


def solution(mesh):
    placed = (
        P("dp", None),
        P(),
        P("dp", None, "tensor"),
        P("dp", None, "tensor"),
        P("dp", None, "tensor"),
        P("dp", None, "tensor"),
        P("dp", None, "tensor"),
        P("dp", None, "tensor"),
        P("tensor", None, "dp"),
        P("tensor", None, "dp"),
    )
    return jax.shard_map(
        shards, mesh=mesh, in_specs=placed, out_specs=P("dp", None), check_vma=False
    )
```
